32 devices in a mesh: ens: 4 (over y, x), fsdp: 2 (over core), model: 4 (over z).
Axes of the slice: x: 2, y: 2, z: 4, core: 2. Of those that a mesh axis runs over, the one named last changes fastest.
Arguments:
- weight_gate: bfloat16 [8192, 8192], P(('ens', 'fsdp'), 'model'), parts along dimension 0, may hold values from -0.125 to 0.125
- low_gate: bfloat16 [8192, 32], P(('ens', 'fsdp')), parts along dimension 0, may hold values from -0.125 to 0.125
- high_gate: bfloat16 [128, 8192], P('ens', 'model'), parts along dimension 0, may hold values from -1 to 1
- weight_up: bfloat16 [8192, 8192], P(('ens', 'fsdp'), 'model'), parts along dimension 0, may hold values from -0.125 to 0.125
- low_up: bfloat16 [8192, 32], P(('ens', 'fsdp')), parts along dimension 0, may hold values from -0.125 to 0.125
- high_up: bfloat16 [128, 8192], P('ens', 'model'), parts along dimension 0, may hold values from -1 to 1
- norm_train: float32 [8192], P(('ens', 'fsdp', 'model')), parts along dimension 0, may hold values from 0.25 to 1.75
- norm_step: float32 [8192], P(('ens', 'fsdp', 'model')), parts along dimension 0, may hold values from -0.3 to 0.3
Outputs:
- final_gate: bfloat16 [32768, 2048], P(('ens', 'model')), parts along dimension 0
- final_up: bfloat16 [32768, 2048], P(('ens', 'model')), parts along dimension 0
- serve_norm: bfloat16 [8192], P('ens'), parts along dimension 0
The draws below stay inside these ranges and needn't reach their ends.
There are 4 independent parts, one for each index of `ens`. The reference program is written for one: setup_inputs(seed, part) draws one part's arguments, and reference() takes and returns one part's arrays. A program takes and returns all parts, laid end to end along the dimension named above; each array names one. Nothing has to cross between parts.
All inputs are finite; a program needn't handle non-finite values.
Results may differ from the reference program's by a relative error of at most 0.001.
Values may be sent and summed in bfloat16 or wider, within the bound.
A program may use at most 128 MiB of HBM per device.

```python
import jax
import jax.numpy as jnp

D_MODEL = 2048
D_INNER = 8192
RANK = 32


def steps_of(own_key, shape, cuts, least, high):
    def one(dim, blocks):
        steps = jax.random.uniform(jax.random.fold_in(jax.random.fold_in(own_key, 6), dim), (blocks,), jnp.float32, least / len(cuts), high / len(cuts))
        return jnp.repeat(jnp.exp(steps), shape[dim] // blocks).reshape((-1,) + (1,) * (len(shape) - dim - 1))

    gain = one(*cuts[0])
    for cut in cuts[1:]:
        gain = gain * one(*cut)
    return gain


def bell_draw(own_key, shape, spread, limit, shards=(), held_as=jnp.bfloat16):
    loudness = steps_of(own_key, shape, shards, -0.22, 0.18) if shards else 1.0
    values = jax.random.normal(own_key, shape, jnp.float32) * spread * loudness
    return jnp.minimum(jnp.maximum(values, -limit), limit).astype(held_as)


def setup_inputs(seed: int = 0, part: int = 0) -> dict:
    keys = jax.random.split(jax.random.key(seed), 9)
    part_keys = jax.random.split(jax.random.fold_in(keys[8], part), 9)
    weight_gate = bell_draw(part_keys[0], (D_MODEL, D_INNER), D_MODEL ** -0.5, 0.125, ((0, 2), (1, 4)))
    low_gate = bell_draw(part_keys[1], (D_MODEL, RANK), D_MODEL ** -0.5, 0.125, ((0, 2),))
    high_gate = bell_draw(part_keys[2], (RANK, D_INNER), RANK ** -0.5, 1.0, ((1, 4),))
    weight_up = bell_draw(part_keys[3], (D_MODEL, D_INNER), D_MODEL ** -0.5, 0.125, ((0, 2), (1, 4)))
    low_up = bell_draw(part_keys[4], (D_MODEL, RANK), D_MODEL ** -0.5, 0.125, ((0, 2),))
    high_up = bell_draw(part_keys[5], (RANK, D_INNER), RANK ** -0.5, 1.0, ((1, 4),))
    norm_train = jnp.clip(1.0 + 0.15 * jax.random.normal(part_keys[6], (D_MODEL,), jnp.float32), 0.25, 1.75)
    norm_step = jnp.clip(jax.random.uniform(part_keys[7], (D_MODEL,), jnp.float32, -0.3, 0.3) * steps_of(part_keys[7], (D_MODEL,), ((0, 8),), -0.4, 0.0), -0.3, 0.3)
    return {"weight_gate": weight_gate, "low_gate": low_gate, "high_gate": high_gate, "weight_up": weight_up, "low_up": low_up, "high_up": high_up, "norm_train": norm_train, "norm_step": norm_step}


mix_rate = 2.0


def reference(weight_gate, low_gate, high_gate, weight_up, low_up, high_up, norm_train, norm_step):
    result_gate = weight_gate.astype(jnp.float32) + mix_rate * jnp.dot(low_gate, high_gate, preferred_element_type=jnp.float32)
    result_up = weight_up.astype(jnp.float32) + mix_rate * jnp.dot(low_up, high_up, preferred_element_type=jnp.float32)
    final_gate = result_gate.T.astype(jnp.bfloat16)
    final_up = result_up.T.astype(jnp.bfloat16)
    serve_norm = (norm_train + norm_step).astype(jnp.bfloat16)
    return final_gate, final_up, serve_norm
```

```python
import functools

import jax
import jax.numpy as jnp
from jax import lax
from jax.experimental import pallas as pl
from jax.experimental.pallas import tpu as pltpu
from jax.sharding import PartitionSpec as P


mix_rate = 2.0
MIB = 2 ** 20
MESH = pl.DeviceIdType.MESH
VMEM, HBM = pl.BlockSpec(memory_space=pltpu.VMEM), pl.BlockSpec(memory_space=pltpu.HBM)
ANY = pl.BlockSpec(memory_space=pl.ANY)

TILE = 256
IN_FLIGHT = 3
EARLY = 2
SHARES = (10, 4, 2)
PLACED = ((0, 1), (2,))


def in_vmem(array):
    return pltpu.with_memory_space_constraint(array, pltpu.VMEM)


def in_hbm(array):
    return pltpu.with_memory_space_constraint(array, pltpu.HBM)


def merge(weight, low, high):
    product = lax.dot_general(
        high, low * mix_rate, (((0,), (0,)), ((), ())), preferred_element_type=jnp.float32
    )
    return (weight.T.astype(jnp.float32) + product).astype(jnp.bfloat16)


def cost(flops, size):
    return pl.CostEstimate(flops=flops, bytes_accessed=size, transcendentals=0)


def own_kernel(sizes, cuts, *refs):
    fsdp, model = sizes
    count = fsdp * model
    ins, norms, norm_all = refs[:6], refs[6:8], refs[8]
    outs = refs[9: 10 + len(cuts)]
    held, low_held, high_held, read_sem, small_sem, keep_sem, send_sem, recv_sem = refs[
        10 + len(cuts):
    ]
    rows, columns = ins[0].shape
    tile = min(rows, TILE)
    steps = rows // tile
    row, column = lax.axis_index("fsdp"), lax.axis_index("model")
    barrier = pltpu.get_barrier_semaphore()

    def peer(shift):
        return {
            "fsdp": lax.rem(row + shift // model, fsdp),
            "model": lax.rem(column + shift % model, model),
        }

    for shift in range(1, count):
        pl.semaphore_signal(barrier, inc=1, device_id=peer(shift), device_id_type=MESH)

    place = row * model + column
    keep = [
        pltpu.make_async_copy(norms[i], norm_all.at[i, place], keep_sem.at[i]) for i in range(2)
    ]
    smalls = [
        [
            pltpu.make_async_copy(ins[3 * i + 1], low_held.at[i], small_sem.at[i, 0]),
            pltpu.make_async_copy(ins[3 * i + 2], high_held.at[i], small_sem.at[i, 1]),
        ]
        for i in range(2)
    ]
    order = [(i, j) for i in (1, 0) for j in range(steps)]
    reads = [
        pltpu.make_async_copy(
            ins[3 * i].at[pl.ds(j * tile, tile)], held.at[i, pl.ds(j * tile, tile)],
            read_sem.at[i, j],
        )
        for i, j in order
    ]
    for copy in smalls[1] + reads[:IN_FLIGHT] + keep + smalls[0]:
        copy.start()

    bounds = [sum(cuts[:k]) for k in range(len(cuts))]
    copies = []
    for n, (i, j) in enumerate(order):
        if n == min(EARLY, len(order) - 1):
            for copy in keep:
                copy.wait()
            pl.semaphore_wait(barrier, count - 1)
            for shift in range(1, count):
                for k in range(2):
                    copies.append(pltpu.make_async_remote_copy(
                        src_ref=norm_all.at[k, place], dst_ref=norm_all.at[k, place],
                        send_sem=send_sem.at[k, shift], recv_sem=recv_sem.at[k, shift],
                        device_id=peer(shift), device_id_type=MESH,
                    ))
                    copies[-1].start()
        if j == 0:
            for copy in smalls[i]:
                copy.wait()
        reads[n].wait()
        if n + IN_FLIGHT < len(reads):
            reads[n + IN_FLIGHT].start()
        low = low_held[i, :, j * tile: (j + 1) * tile]
        for start, size, out in (
            [(0, columns, outs[-1])] if i == 0 else zip(bounds, cuts, outs)
        ):
            width = min(size, TILE)
            for first in range(0, size, width):
                piece = slice(start + first, start + first + width)
                out[first: first + width, j * tile: (j + 1) * tile] = merge(
                    held[i, j * tile: (j + 1) * tile, piece], low, high_held[i, :, piece]
                )
    for copy in copies:
        copy.wait()


def own_part(sizes, cuts, groups, norms):
    fsdp, model = sizes
    rows, columns = groups[0][0].shape
    rank = groups[0][1].shape[0]
    count, steps = fsdp * model, rows // min(rows, TILE)
    dma = pltpu.SemaphoreType.DMA
    return pl.pallas_call(
        functools.partial(own_kernel, sizes, cuts),
        out_shape=[pltpu.VMEM((2, count) + norms[0].shape, jnp.float32)]
        + [pltpu.VMEM((cut, rows), jnp.bfloat16) for cut in cuts + (columns,)],
        in_specs=[HBM] * 8,
        out_specs=[VMEM] * (2 + len(cuts)),
        scratch_shapes=[
            pltpu.VMEM((2, rows, columns), jnp.bfloat16),
            pltpu.VMEM((2, rank, rows), jnp.bfloat16),
            pltpu.VMEM((2, rank, columns), jnp.bfloat16),
            dma((2, steps)), dma((2, 2)), dma((2,)), dma((2, count)), dma((2, count)),
        ],
        compiler_params=pltpu.CompilerParams(
            collective_id=0, has_side_effects=True, vmem_limit_bytes=12 * MIB
        ),
        cost_estimate=cost(4 * rows * columns * rank, 4 * rows * columns),
    )(*[in_hbm(a) for group in groups for a in group], *[in_hbm(a) for a in norms])


def column_of(step, fsdp, rows):
    source = lax.rem(lax.axis_index("fsdp") + (fsdp - step), fsdp)
    return pl.ds(pl.multiple_of(source * rows, rows), rows)


def rest_kernel(fsdp, cuts, *refs):
    norm_all, high, own_gate = refs[:3]
    own_up, theirs = refs[3: 3 + len(cuts)], refs[3 + len(cuts): -6]
    out_gate, out_up, serve_norm, made, own_sem, write_sem = refs[-6:]
    columns, rows = own_gate.shape
    tile = min(columns, TILE)
    mine = column_of(0, fsdp, rows)

    copies = [pltpu.make_async_copy(own_gate, out_gate.at[:, mine], own_sem.at[0])]
    start = 0
    for k, block in enumerate(own_up):
        copies.append(pltpu.make_async_copy(
            block, out_up.at[pl.ds(start, cuts[k]), mine], own_sem.at[k + 1]
        ))
        start += cuts[k]
    for copy in copies:
        copy.start()
    for step in range(1, fsdp):
        weight, low = theirs[2 * step - 2: 2 * step]
        for j in range(columns // tile):
            piece = pl.ds(j * tile, tile)
            made[step - 1, piece] = merge(weight[:, piece], low[...], high[:, piece])
            copies.append(pltpu.make_async_copy(
                made.at[step - 1, piece], out_gate.at[piece, column_of(step, fsdp, rows)],
                write_sem.at[step - 1, j],
            ))
            copies[-1].start()
    size = norm_all.shape[-1]
    for k in range(norm_all.shape[1]):
        total = norm_all[0, k, 0, :] + norm_all[1, k, 0, :]
        serve_norm[pl.ds(k * size, size)] = total.astype(serve_norm.dtype)
    for copy in copies:
        copy.wait()


def rest(fsdp, norm_all, high, own_gate, own_up, theirs):
    columns, rows = own_gate.shape
    cuts = tuple(a.shape[0] for a in own_up)
    full = jax.ShapeDtypeStruct((columns, rows * fsdp), jnp.bfloat16)
    dma = pltpu.SemaphoreType.DMA
    operands = [norm_all, high, own_gate, *own_up, *theirs]
    return pl.pallas_call(
        functools.partial(rest_kernel, fsdp, cuts),
        out_shape=[full, full, jax.ShapeDtypeStruct((norm_all[0].size,), jnp.bfloat16)],
        in_specs=[VMEM] * len(operands),
        out_specs=[ANY, ANY, VMEM],
        scratch_shapes=[
            pltpu.VMEM((fsdp - 1, columns, rows), jnp.bfloat16),
            dma((1 + len(cuts),)), dma((fsdp - 1, columns // min(columns, TILE))),
        ],
        compiler_params=pltpu.CompilerParams(vmem_limit_bytes=12 * MIB),
        cost_estimate=cost(2 * rows * columns * high.shape[0], 6 * rows * columns),
    )(*[in_vmem(a) for a in operands])


def place_kernel(fsdp, starts, *refs):
    blocks, out, sem = refs[: -3], refs[-2], refs[-1]
    copies = []
    for k, block in enumerate(blocks):
        start, step = starts[k]
        size, rows = block.shape
        copies.append(pltpu.make_async_copy(
            block, out.at[pl.ds(start, size), column_of(step, fsdp, rows)], sem.at[k]
        ))
        copies[-1].start()
    for copy in copies:
        copy.wait()


def place(fsdp, starts, blocks, held):
    size = sum(a.size for a in blocks)
    return pl.pallas_call(
        functools.partial(place_kernel, fsdp, starts),
        out_shape=jax.ShapeDtypeStruct(held.shape, held.dtype),
        in_specs=[VMEM] * len(blocks) + [ANY],
        out_specs=ANY,
        scratch_shapes=[pltpu.SemaphoreType.DMA((len(blocks),))],
        input_output_aliases={len(blocks): 0},
        compiler_params=pltpu.CompilerParams(vmem_limit_bytes=MIB),
        cost_estimate=cost(32 * size, 2 * size),
    )(*[in_vmem(a) for a in blocks], held)


def send(array, fsdp):
    return [
        lax.ppermute(array, "fsdp", [(i, (i + step) % fsdp) for i in range(fsdp)])
        for step in range(1, fsdp)
    ]


def body(sizes, weight_gate, low_gate, high_gate, weight_up, low_up, high_up, norm_train, norm_step):
    fsdp, _ = sizes
    low_gate, low_up = low_gate.T, low_up.T
    its_gate = send(in_hbm(weight_gate), fsdp)
    its_low = send(in_hbm(low_gate), fsdp)
    columns = weight_up.shape[1]
    cuts = tuple(columns * share // 16 for share in SHARES)
    groups = [(weight_gate, low_gate, high_gate), (weight_up, low_up, high_up)]
    norms = [norm_train.reshape(1, -1), norm_step.reshape(1, -1)]
    norm_all, *made = own_part(sizes, cuts, groups, norms)
    own_up, own_gate = made[:-1], made[-1]
    its_up = [send(a, fsdp) for a in own_up]
    theirs = [a for pair in zip(its_gate, its_low) for a in pair]
    gate, up, serve_norm = rest(fsdp, norm_all, high_gate, own_gate, own_up, theirs)
    for group in PLACED:
        ends = [(k, step) for k in group for step in range(1, fsdp)]
        up = place(
            fsdp, tuple((sum(cuts[:k]), step) for k, step in ends),
            [its_up[k][step - 1] for k, step in ends], up,
        )
    return gate, up, serve_norm


def solution(mesh):
    whole = P(("ens", "fsdp", "model"))
    rows, thin, high = P(("ens", "fsdp"), "model"), P(("ens", "fsdp"), None), P("ens", "model")
    return jax.shard_map(
        functools.partial(body, (mesh.shape["fsdp"], mesh.shape["model"])),
        mesh=mesh,
        in_specs=(rows, thin, high, rows, thin, high, whole, whole),
        out_specs=(P(("ens", "model"), None), P(("ens", "model"), None), P("ens")),
        check_vma=False,
    )
```

```python
import functools

import jax
import jax.numpy as jnp
from jax import lax
from jax.experimental import pallas as pl
from jax.experimental.pallas import tpu as pltpu
from jax.sharding import PartitionSpec as P


mix_rate = 2.0
MIB = 2 ** 20
MESH = pl.DeviceIdType.MESH
VMEM, HBM = pl.BlockSpec(memory_space=pltpu.VMEM), pl.BlockSpec(memory_space=pltpu.HBM)
ANY = pl.BlockSpec(memory_space=pl.ANY)

TILE = 256
CUTS = ((2, 2), (1, 1, 2))
IN_FLIGHT = 3
EARLY = 2


def in_vmem(array):
    return pltpu.with_memory_space_constraint(array, pltpu.VMEM)


def in_hbm(array):
    return pltpu.with_memory_space_constraint(array, pltpu.HBM)


def merge(weight, low, high):
    product = lax.dot_general(
        high, low * mix_rate, (((0,), (0,)), ((), ())), preferred_element_type=jnp.float32
    )
    return (weight.T.astype(jnp.float32) + product).astype(jnp.bfloat16)


def cost(flops, size):
    return pl.CostEstimate(flops=flops, bytes_accessed=size, transcendentals=0)


def blocks_of(rows):
    order = []
    for i in (1, 0):
        start = 0
        for cut in CUTS[i] if rows % 512 == 0 else (4,):
            order.append((i, start, rows * cut // 4))
            start += rows * cut // 4
    return order


def own_kernel(sizes, *refs):
    fsdp, model = sizes
    count = fsdp * model
    ins, norms, (norm_all, its_low, *outs) = refs[:6], refs[6:8], refs[8:12]
    held, low_held, high_held, read_sem, small_sem, keep_sem, send_sem, recv_sem = refs[12:20]
    low_send, low_recv = refs[20:]
    rows, columns = ins[0].shape
    row, column = lax.axis_index("fsdp"), lax.axis_index("model")
    barrier = pltpu.get_barrier_semaphore()

    def peer(shift):
        return {
            "fsdp": lax.rem(row + shift // model, fsdp),
            "model": lax.rem(column + shift % model, model),
        }

    for shift in range(1, count):
        pl.semaphore_signal(barrier, inc=1, device_id=peer(shift), device_id_type=MESH)

    place = row * model + column
    keep = [
        pltpu.make_async_copy(norms[i], norm_all.at[i, place], keep_sem.at[i]) for i in range(2)
    ]
    smalls = [
        [
            pltpu.make_async_copy(ins[3 * i + 1], low_held.at[i], small_sem.at[i, 0]),
            pltpu.make_async_copy(ins[3 * i + 2], high_held.at[i], small_sem.at[i, 1]),
        ]
        for i in range(2)
    ]
    order = blocks_of(rows)
    reads = [
        pltpu.make_async_copy(
            ins[3 * i].at[pl.ds(start, size)], held.at[i, pl.ds(start, size)], read_sem.at[n]
        )
        for n, (i, start, size) in enumerate(order)
    ]
    for copy in smalls[1] + reads[:IN_FLIGHT] + keep + smalls[0]:
        copy.start()

    copies = []
    ready = set()
    ahead = IN_FLIGHT
    for n, (i, start, size) in enumerate(order):
        if n == EARLY:
            for copy in reads[ahead:]:
                copy.start()
            ahead = len(reads)
            for k in {0, 1} - ready:
                for copy in smalls[k]:
                    copy.wait()
            ready = {0, 1}
            for copy in keep:
                copy.wait()
            pl.semaphore_wait(barrier, count - 1)
            for shift in range(1, count):
                for k in range(2):
                    copies.append(pltpu.make_async_remote_copy(
                        src_ref=norm_all.at[k, place], dst_ref=norm_all.at[k, place],
                        send_sem=send_sem.at[k, shift], recv_sem=recv_sem.at[k, shift],
                        device_id=peer(shift), device_id_type=MESH,
                    ))
            for step in range(1, fsdp):
                for k in range(2):
                    copies.append(pltpu.make_async_remote_copy(
                        src_ref=low_held.at[k], dst_ref=its_low.at[step - 1, k],
                        send_sem=low_send.at[step - 1, k], recv_sem=low_recv.at[step - 1, k],
                        device_id=peer(step * model), device_id_type=MESH,
                    ))
            for copy in copies:
                copy.start()
        if i not in ready:
            for copy in smalls[i]:
                copy.wait()
            ready.add(i)
        reads[n].wait()
        if ahead < len(reads):
            reads[ahead].start()
            ahead += 1
        band = slice(start, start + size)
        for first in range(0, columns, min(columns, TILE)):
            piece = slice(first, first + min(columns, TILE))
            outs[i][piece, band] = merge(
                held[i, band, piece], low_held[i, :, band], high_held[i, :, piece]
            )
    for copy in copies:
        copy.wait()


def own_part(sizes, groups, norms):
    fsdp, model = sizes
    rows, columns = groups[0][0].shape
    rank = groups[0][1].shape[0]
    count, dma = fsdp * model, pltpu.SemaphoreType.DMA
    return pl.pallas_call(
        functools.partial(own_kernel, sizes),
        out_shape=[
            pltpu.VMEM((2, count) + norms[0].shape, jnp.float32),
            pltpu.VMEM((fsdp - 1, 2, rank, rows), jnp.bfloat16),
            pltpu.VMEM((columns, rows), jnp.bfloat16),
            pltpu.VMEM((columns, rows), jnp.bfloat16),
        ],
        in_specs=[HBM] * 8,
        out_specs=[VMEM] * 4,
        scratch_shapes=[
            pltpu.VMEM((2, rows, columns), jnp.bfloat16),
            pltpu.VMEM((2, rank, rows), jnp.bfloat16),
            pltpu.VMEM((2, rank, columns), jnp.bfloat16),
            dma((len(blocks_of(rows)),)), dma((2, 2)), dma((2,)), dma((2, count)), dma((2, count)),
            dma((fsdp - 1, 2)), dma((fsdp - 1, 2)),
        ],
        compiler_params=pltpu.CompilerParams(
            collective_id=0, has_side_effects=True, vmem_limit_bytes=12 * MIB
        ),
        cost_estimate=cost(4 * rows * columns * rank, 4 * rows * columns),
    )(*[in_hbm(a) for group in groups for a in group], *[in_hbm(a) for a in norms])


def column_of(step, fsdp, rows):
    source = lax.rem(lax.axis_index("fsdp") + (fsdp - step), fsdp)
    return pl.ds(pl.multiple_of(source * rows, rows), rows)


def merge_theirs(fsdp, index, weights, its_low, high, out, made, sem):
    copies = []
    for step, weight in enumerate(weights, 1):
        rows, columns = weight.shape
        tile = min(columns, TILE)
        for j in range(columns // tile):
            piece = pl.ds(j * tile, tile)
            made[step - 1, piece] = merge(weight[:, piece], its_low[step - 1, index], high[:, piece])
            copies.append(pltpu.make_async_copy(
                made.at[step - 1, piece], out.at[piece, column_of(step, fsdp, rows)],
                sem.at[step - 1, j],
            ))
            copies[-1].start()
    return copies


def gate_kernel(fsdp, norm_all, its_low, own_gate, own_up, high, *refs):
    weights, (out_gate, out_up, serve_norm, made, own_sem, write_sem) = refs[:-6], refs[-6:]
    mine = column_of(0, fsdp, own_gate.shape[1])
    copies = [
        pltpu.make_async_copy(own_gate, out_gate.at[:, mine], own_sem.at[0]),
        pltpu.make_async_copy(own_up, out_up.at[:, mine], own_sem.at[1]),
    ]
    for copy in copies:
        copy.start()
    copies += merge_theirs(fsdp, 0, weights, its_low, high, out_gate, made, write_sem)
    size = norm_all.shape[-1]
    for k in range(norm_all.shape[1]):
        total = norm_all[0, k, 0, :] + norm_all[1, k, 0, :]
        serve_norm[pl.ds(k * size, size)] = total.astype(serve_norm.dtype)
    for copy in copies:
        copy.wait()


def up_kernel(fsdp, its_low, high, *refs):
    weights, (_, out, made, write_sem) = refs[:-4], refs[-4:]
    for copy in merge_theirs(fsdp, 1, weights, its_low, high, out, made, write_sem):
        copy.wait()


def theirs_scratch(fsdp, columns, rows):
    return [
        pltpu.VMEM((fsdp - 1, columns, rows), jnp.bfloat16),
        pltpu.SemaphoreType.DMA((fsdp - 1, columns // min(columns, TILE))),
    ]


def gate_part(fsdp, norm_all, its_low, own_gate, own_up, high, weights):
    columns, rows = own_gate.shape
    full = jax.ShapeDtypeStruct((columns, rows * fsdp), jnp.bfloat16)
    operands = [norm_all, its_low, own_gate, own_up, high, *weights]
    made, sem = theirs_scratch(fsdp, columns, rows)
    return pl.pallas_call(
        functools.partial(gate_kernel, fsdp),
        out_shape=[full, full, jax.ShapeDtypeStruct((norm_all[0].size,), jnp.bfloat16)],
        in_specs=[VMEM] * len(operands),
        out_specs=[ANY, ANY, VMEM],
        scratch_shapes=[made, pltpu.SemaphoreType.DMA((2,)), sem],
        compiler_params=pltpu.CompilerParams(vmem_limit_bytes=12 * MIB),
        cost_estimate=cost(2 * rows * columns * high.shape[0], 6 * rows * columns),
    )(*[in_vmem(a) for a in operands])


def up_part(fsdp, its_low, high, weights, held):
    rows, columns = weights[0].shape
    operands = [its_low, high, *weights]
    return pl.pallas_call(
        functools.partial(up_kernel, fsdp),
        out_shape=jax.ShapeDtypeStruct(held.shape, held.dtype),
        in_specs=[VMEM] * len(operands) + [ANY],
        out_specs=ANY,
        scratch_shapes=theirs_scratch(fsdp, columns, rows),
        input_output_aliases={len(operands): 0},
        compiler_params=pltpu.CompilerParams(vmem_limit_bytes=12 * MIB),
        cost_estimate=cost(2 * rows * columns * high.shape[0], 2 * rows * columns),
    )(*[in_vmem(a) for a in operands], held)


def send(array, fsdp):
    return [
        lax.ppermute(array, "fsdp", [(i, (i + step) % fsdp) for i in range(fsdp)])
        for step in range(1, fsdp)
    ]


def body(sizes, weight_gate, low_gate, high_gate, weight_up, low_up, high_up, norm_train, norm_step):
    fsdp, _ = sizes
    low_gate, low_up = low_gate.T, low_up.T
    its_gate = send(in_hbm(weight_gate), fsdp)
    its_up = send(in_hbm(weight_up), fsdp)
    groups = [(weight_gate, low_gate, high_gate), (weight_up, low_up, high_up)]
    norm_all, its_low, own_gate, own_up = own_part(
        sizes, groups, [norm_train.reshape(1, -1), norm_step.reshape(1, -1)]
    )
    gate, up, serve_norm = gate_part(
        fsdp, norm_all, its_low, own_gate, own_up, high_gate, its_gate
    )
    return gate, up_part(fsdp, its_low, high_up, its_up, up), serve_norm


def solution(mesh):
    whole = P(("ens", "fsdp", "model"))
    rows, thin, high = P(("ens", "fsdp"), "model"), P(("ens", "fsdp"), None), P("ens", "model")
    return jax.shard_map(
        functools.partial(body, (mesh.shape["fsdp"], mesh.shape["model"])),
        mesh=mesh,
        in_specs=(rows, thin, high, rows, thin, high, whole, whole),
        out_specs=(P(("ens", "model"), None), P(("ens", "model"), None), P("ens")),
        check_vma=False,
    )
```

```python
import functools

import jax
import jax.numpy as jnp
from jax import lax
from jax.experimental import pallas as pl
from jax.experimental.pallas import tpu as pltpu
from jax.sharding import PartitionSpec as P


mix_rate = 2.0
MIB = 2 ** 20
MESH = pl.DeviceIdType.MESH
VMEM, HBM = pl.BlockSpec(memory_space=pltpu.VMEM), pl.BlockSpec(memory_space=pltpu.HBM)
ANY = pl.BlockSpec(memory_space=pl.ANY)

TILE = 256
CUTS = ((2, 2), (1, 1, 2))
IN_FLIGHT = 3
EARLY = 2
SHARES = (3, 1)


def in_vmem(array):
    return pltpu.with_memory_space_constraint(array, pltpu.VMEM)


def in_hbm(array):
    return pltpu.with_memory_space_constraint(array, pltpu.HBM)


def merge(weight, low, high):
    product = lax.dot_general(
        high, low * mix_rate, (((0,), (0,)), ((), ())), preferred_element_type=jnp.float32
    )
    return (weight.T.astype(jnp.float32) + product).astype(jnp.bfloat16)


def cost(flops, size):
    return pl.CostEstimate(flops=flops, bytes_accessed=size, transcendentals=0)


def blocks_of(rows):
    order = []
    for i in (1, 0):
        start = 0
        for cut in CUTS[i] if rows % 512 == 0 else (4,):
            order.append((i, start, rows * cut // 4))
            start += rows * cut // 4
    return order


def own_kernel(sizes, cuts, *refs):
    fsdp, model = sizes
    ins, norms, (norm_all, pack, own_gate, *own_up) = refs[:6], refs[6:8], refs[8: 11 + len(cuts)]
    held, low_held, high_held, read_sem, small_sem, keep_sem, send_sem, recv_sem = refs[
        11 + len(cuts):
    ]
    rows, _ = ins[0].shape
    row, column = lax.axis_index("fsdp"), lax.axis_index("model")
    barrier = pltpu.get_barrier_semaphore()

    def peer(shift):
        return {
            "fsdp": lax.rem(row + shift // (model - 1), fsdp),
            "model": lax.rem(column + 1 + shift % (model - 1), model),
        }

    peers = range(fsdp * (model - 1))
    for shift in peers:
        pl.semaphore_signal(barrier, inc=1, device_id=peer(shift), device_id_type=MESH)

    place = row * model + column
    keep = [
        pltpu.make_async_copy(norms[i], norm_all.at[i, place], keep_sem.at[i]) for i in range(2)
    ]
    smalls = [
        [
            pltpu.make_async_copy(ins[3 * i + 1], low_held.at[i], small_sem.at[i, 0]),
            pltpu.make_async_copy(ins[3 * i + 2], high_held.at[i], small_sem.at[i, 1]),
        ]
        for i in range(2)
    ]
    order = blocks_of(rows)
    reads = [
        pltpu.make_async_copy(
            ins[3 * i].at[pl.ds(start, size)], held.at[i, pl.ds(start, size)], read_sem.at[n]
        )
        for n, (i, start, size) in enumerate(order)
    ]
    for copy in smalls[1] + reads[:IN_FLIGHT] + keep + smalls[0]:
        copy.start()

    copies = []
    ready = set()
    ahead = IN_FLIGHT
    for n, (i, start, size) in enumerate(order):
        if n == EARLY:
            for copy in reads[ahead:]:
                copy.start()
            ahead = len(reads)
            for k in {0, 1} - ready:
                for copy in smalls[k]:
                    copy.wait()
            ready = {0, 1}
            for copy in keep:
                copy.wait()
            pl.semaphore_wait(barrier, len(peers))
            for shift in peers:
                for k in range(2):
                    copies.append(pltpu.make_async_remote_copy(
                        src_ref=norm_all.at[k, place], dst_ref=norm_all.at[k, place],
                        send_sem=send_sem.at[k, shift], recv_sem=recv_sem.at[k, shift],
                        device_id=peer(shift), device_id_type=MESH,
                    ))
            for copy in copies:
                copy.start()
        if i not in ready:
            for copy in smalls[i]:
                copy.wait()
            ready.add(i)
        reads[n].wait()
        if ahead < len(reads):
            reads[ahead].start()
            ahead += 1
        band = slice(start, start + size)
        first = 0
        for out in own_up if i else [own_gate]:
            tile = min(out.shape[0], TILE)
            for within in range(0, out.shape[0], tile):
                piece = slice(first, first + tile)
                out[within: within + tile, band] = merge(
                    held[i, band, piece], low_held[i, :, band], high_held[i, :, piece]
                )
                first += tile
    rank, size = low_held.shape[1], norm_all.shape[-1]
    pack[:rank] = low_held[0]
    pack[rank:, :size] = jnp.broadcast_to(
        norm_all[0, place] + norm_all[1, place], (pack.shape[0] - rank, size)
    ).astype(pack.dtype)
    for copy in copies:
        copy.wait()


def own_part(sizes, cuts, groups, norms):
    fsdp, model = sizes
    rows, columns = groups[0][0].shape
    rank = groups[0][1].shape[0]
    count, dma = fsdp * model, pltpu.SemaphoreType.DMA
    return pl.pallas_call(
        functools.partial(own_kernel, sizes, cuts),
        out_shape=[
            pltpu.VMEM((2, count) + norms[0].shape, jnp.float32),
            pltpu.VMEM((rank + 16, rows), jnp.bfloat16),
        ] + [pltpu.VMEM((cut, rows), jnp.bfloat16) for cut in (columns,) + cuts],
        in_specs=[HBM] * 8,
        out_specs=[VMEM] * (3 + len(cuts)),
        scratch_shapes=[
            pltpu.VMEM((2, rows, columns), jnp.bfloat16),
            pltpu.VMEM((2, rank, rows), jnp.bfloat16),
            pltpu.VMEM((2, rank, columns), jnp.bfloat16),
            dma((len(blocks_of(rows)),)), dma((2, 2)), dma((2,)), dma((2, count)), dma((2, count)),
        ],
        compiler_params=pltpu.CompilerParams(
            collective_id=0, has_side_effects=True, vmem_limit_bytes=12 * MIB
        ),
        cost_estimate=cost(4 * rows * columns * rank, 4 * rows * columns),
    )(*[in_hbm(a) for group in groups for a in group], *[in_hbm(a) for a in norms])


def column_of(step, fsdp, rows):
    source = lax.rem(lax.axis_index("fsdp") + (fsdp - step), fsdp)
    return pl.ds(pl.multiple_of(source * rows, rows), rows)


def rest_kernel(fsdp, model, count, *refs):
    norm_all, high, own_gate = refs[:3]
    own_up, theirs = refs[3: 3 + count], refs[3 + count: -7]
    out_gate, out_up, serve_norm, made, gain, own_sem, write_sem = refs[-7:]
    columns, rows = own_gate.shape
    rank, tile = high.shape[0], min(columns, TILE)
    mine = column_of(0, fsdp, rows)

    copies = [pltpu.make_async_copy(own_gate, out_gate.at[:, mine], own_sem.at[0])]
    start = 0
    for k, block in enumerate(own_up):
        copies.append(pltpu.make_async_copy(
            block, out_up.at[pl.ds(start, block.shape[0]), mine], own_sem.at[k + 1]
        ))
        start += block.shape[0]
    for copy in copies:
        copy.start()
    for step in range(1, fsdp):
        weight, pack = theirs[2 * step - 2: 2 * step]
        for j in range(columns // tile):
            piece = pl.ds(j * tile, tile)
            made[step - 1, piece] = merge(weight[:, piece], pack[:rank], high[:, piece])
            copies.append(pltpu.make_async_copy(
                made.at[step - 1, piece], out_gate.at[piece, column_of(step, fsdp, rows)],
                write_sem.at[step - 1, j],
            ))
            copies[-1].start()

    gain[...] = norm_all[0] + norm_all[1]
    size = gain.shape[-1]
    for step in range(1, fsdp):
        source = lax.rem(lax.axis_index("fsdp") + (fsdp - step), fsdp)
        pack = theirs[2 * step - 1]
        gain[source * model + lax.axis_index("model")] = pack[rank:, :size].astype(jnp.float32)[:1]
    for k in range(gain.shape[0]):
        serve_norm[pl.ds(k * size, size)] = gain[k, 0, :].astype(serve_norm.dtype)
    for copy in copies:
        copy.wait()


def rest(sizes, norm_all, high, own_gate, own_up, theirs):
    fsdp, model = sizes
    columns, rows = own_gate.shape
    full = jax.ShapeDtypeStruct((columns, rows * fsdp), jnp.bfloat16)
    dma = pltpu.SemaphoreType.DMA
    operands = [norm_all, high, own_gate, *own_up, *theirs]
    return pl.pallas_call(
        functools.partial(rest_kernel, fsdp, model, len(own_up)),
        out_shape=[full, full, jax.ShapeDtypeStruct((norm_all[0].size,), jnp.bfloat16)],
        in_specs=[VMEM] * len(operands),
        out_specs=[ANY, ANY, VMEM],
        scratch_shapes=[
            pltpu.VMEM((fsdp - 1, columns, rows), jnp.bfloat16),
            pltpu.VMEM(norm_all.shape[1:], jnp.float32),
            dma((1 + len(own_up),)), dma((fsdp - 1, columns // min(columns, TILE))),
        ],
        compiler_params=pltpu.CompilerParams(vmem_limit_bytes=12 * MIB),
        cost_estimate=cost(2 * rows * columns * high.shape[0], 6 * rows * columns),
    )(*[in_vmem(a) for a in operands])


def place_kernel(fsdp, start, *refs):
    blocks, (_, out, sem) = refs[:-3], refs[-3:]
    copies = []
    for step, block in enumerate(blocks, 1):
        size, rows = block.shape
        copies.append(pltpu.make_async_copy(
            block, out.at[pl.ds(start, size), column_of(step, fsdp, rows)], sem.at[step - 1]
        ))
        copies[-1].start()
    for copy in copies:
        copy.wait()


def place(fsdp, start, blocks, held):
    size = sum(a.size for a in blocks)
    return pl.pallas_call(
        functools.partial(place_kernel, fsdp, start),
        out_shape=jax.ShapeDtypeStruct(held.shape, held.dtype),
        in_specs=[VMEM] * len(blocks) + [ANY],
        out_specs=ANY,
        scratch_shapes=[pltpu.SemaphoreType.DMA((len(blocks),))],
        input_output_aliases={len(blocks): 0},
        compiler_params=pltpu.CompilerParams(vmem_limit_bytes=MIB),
        cost_estimate=cost(32 * size, 2 * size),
    )(*[in_vmem(a) for a in blocks], held)


def send(array, fsdp):
    return [
        lax.ppermute(array, "fsdp", [(i, (i + step) % fsdp) for i in range(fsdp)])
        for step in range(1, fsdp)
    ]


def body(sizes, weight_gate, low_gate, high_gate, weight_up, low_up, high_up, norm_train, norm_step):
    fsdp, _ = sizes
    low_gate, low_up = low_gate.T, low_up.T
    its_gate = send(in_hbm(weight_gate), fsdp)
    columns = weight_up.shape[1]
    cuts = tuple(columns * share // 4 for share in SHARES)
    groups = [(weight_gate, low_gate, high_gate), (weight_up, low_up, high_up)]
    norms = [norm_train.reshape(1, -1), norm_step.reshape(1, -1)]
    norm_all, pack, own_gate, *own_up = own_part(sizes, cuts, groups, norms)
    its_pack = send(pack, fsdp)
    its_up = [send(a, fsdp) for a in own_up]
    theirs = [a for pair in zip(its_gate, its_pack) for a in pair]
    gate, up, serve_norm = rest(sizes, norm_all, high_gate, own_gate, own_up, theirs)
    start = 0
    for cut, blocks in zip(cuts, its_up):
        up = place(fsdp, start, blocks, up)
        start += cut
    return gate, up, serve_norm


def solution(mesh):
    whole = P(("ens", "fsdp", "model"))
    rows, thin, high = P(("ens", "fsdp"), "model"), P(("ens", "fsdp"), None), P("ens", "model")
    return jax.shard_map(
        functools.partial(body, (mesh.shape["fsdp"], mesh.shape["model"])),
        mesh=mesh,
        in_specs=(rows, thin, high, rows, thin, high, whole, whole),
        out_specs=(P(("ens", "model"), None), P(("ens", "model"), None), P("ens")),
        check_vma=False,
    )
```

```python
import functools

import jax
import jax.numpy as jnp
from jax import lax
from jax.experimental import pallas as pl
from jax.experimental.pallas import tpu as pltpu
from jax.sharding import PartitionSpec as P


mix_rate = 2.0
MIB = 2 ** 20
MESH = pl.DeviceIdType.MESH
VMEM, HBM = pl.BlockSpec(memory_space=pltpu.VMEM), pl.BlockSpec(memory_space=pltpu.HBM)
ANY = pl.BlockSpec(memory_space=pl.ANY)

TILE = 256
CUTS = ((2, 2), (1, 1, 2))
IN_FLIGHT = 3
SHARES = (3, 1)
EXTRA = 16


def in_vmem(array):
    return pltpu.with_memory_space_constraint(array, pltpu.VMEM)


def in_hbm(array):
    return pltpu.with_memory_space_constraint(array, pltpu.HBM)


def merge(weight, low, high):
    product = lax.dot_general(
        high, low * mix_rate, (((0,), (0,)), ((), ())), preferred_element_type=jnp.float32
    )
    return (weight.T.astype(jnp.float32) + product).astype(jnp.bfloat16)


def cost(flops, size):
    return pl.CostEstimate(flops=flops, bytes_accessed=size, transcendentals=0)


def blocks_of(rows):
    order = []
    for i in (1, 0):
        start = 0
        for cut in CUTS[i] if rows % 512 == 0 else (4,):
            order.append((i, start, rows * cut // 4))
            start += rows * cut // 4
    return order


def own_kernel(sizes, cuts, *refs):
    fsdp, model = sizes
    ins, norms, (norm_all, own_gate, *own_up) = refs[:6], refs[6:8], refs[8: 10 + len(cuts)]
    held, low_held, high_held, read_sem, small_sem, keep_sem, send_sem, recv_sem = refs[
        10 + len(cuts):
    ]
    rows, columns = ins[0].shape
    row, column = lax.axis_index("fsdp"), lax.axis_index("model")
    barrier = pltpu.get_barrier_semaphore()

    def peer(shift):
        return {
            "fsdp": lax.rem(row + shift // (model - 1), fsdp),
            "model": lax.rem(column + 1 + shift % (model - 1), model),
        }

    peers = range(fsdp * (model - 1))
    for shift in peers:
        pl.semaphore_signal(barrier, inc=1, device_id=peer(shift), device_id_type=MESH)

    place = row * model + column
    keep = [
        pltpu.make_async_copy(norms[i], norm_all.at[i, place], keep_sem.at[i]) for i in range(2)
    ]
    smalls = [
        [
            pltpu.make_async_copy(ins[3 * i + 1], low_held.at[i], small_sem.at[i, 0]),
            pltpu.make_async_copy(ins[3 * i + 2], high_held.at[i], small_sem.at[i, 1]),
        ]
        for i in range(2)
    ]
    order = blocks_of(rows)
    reads = [
        pltpu.make_async_copy(
            ins[3 * i].at[pl.ds(start, size)], held.at[i, pl.ds(start, size)], read_sem.at[n]
        )
        for n, (i, start, size) in enumerate(order)
    ]
    for copy in smalls[1] + reads[:IN_FLIGHT] + keep + smalls[0]:
        copy.start()

    def pieces():
        return [
            pltpu.make_async_remote_copy(
                src_ref=norm_all.at[k, place], dst_ref=norm_all.at[k, place],
                send_sem=send_sem.at[k, shift], recv_sem=recv_sem.at[k, shift],
                device_id=peer(shift), device_id_type=MESH,
            )
            for shift in peers for k in range(2)
        ]

    moment = jnp.maximum(len(order) - 2 * len(order) * column // model, 0)

    def exchange(n):
        @pl.when(moment == n)
        def _():
            pl.semaphore_wait(barrier, len(peers))
            for copy in pieces():
                copy.start()

    for copy in keep:
        copy.wait()
    ahead = IN_FLIGHT
    ready = set()
    for n, (i, start, size) in enumerate(order):
        exchange(n)
        if i not in ready:
            for copy in smalls[i]:
                copy.wait()
            ready.add(i)
        reads[n].wait()
        if ahead < len(reads):
            reads[ahead].start()
            ahead += 1
        band = slice(start, start + size)
        first = 0
        for k, size in enumerate(cuts if i else [columns]):
            out, tile = (own_up[k] if i else own_gate), min(size, TILE)
            for within in range(0, size, tile):
                piece = slice(first, first + tile)
                out[within: within + tile, band] = merge(
                    held[i, band, piece], low_held[i, :, band], high_held[i, :, piece]
                )
                first += tile
    exchange(len(order))
    total = norm_all[0, place] + norm_all[1, place]
    own_up[0][cuts[0]:, : total.shape[-1]] = jnp.broadcast_to(
        total, (own_up[0].shape[0] - cuts[0], total.shape[-1])
    ).astype(jnp.bfloat16)
    for copy in pieces():
        copy.wait()


def own_part(sizes, cuts, groups, norms):
    fsdp, model = sizes
    rows, columns = groups[0][0].shape
    rank = groups[0][1].shape[0]
    count, dma = fsdp * model, pltpu.SemaphoreType.DMA
    return pl.pallas_call(
        functools.partial(own_kernel, sizes, cuts),
        out_shape=[
            pltpu.VMEM((2, count) + norms[0].shape, jnp.float32),
        ] + [
            pltpu.VMEM((cut, rows), jnp.bfloat16)
            for cut in (columns, cuts[0] + EXTRA) + cuts[1:]
        ],
        in_specs=[HBM] * 8,
        out_specs=[VMEM] * (2 + len(cuts)),
        scratch_shapes=[
            pltpu.VMEM((2, rows, columns), jnp.bfloat16),
            pltpu.VMEM((2, rank, rows), jnp.bfloat16),
            pltpu.VMEM((2, rank, columns), jnp.bfloat16),
            dma((len(blocks_of(rows)),)), dma((2, 2)), dma((2,)), dma((2, count)), dma((2, count)),
        ],
        compiler_params=pltpu.CompilerParams(
            collective_id=0, has_side_effects=True, vmem_limit_bytes=12 * MIB
        ),
        cost_estimate=cost(4 * rows * columns * rank, 4 * rows * columns),
    )(*[in_hbm(a) for group in groups for a in group], *[in_hbm(a) for a in norms])


def column_of(step, fsdp, rows):
    source = lax.rem(lax.axis_index("fsdp") + (fsdp - step), fsdp)
    return pl.ds(pl.multiple_of(source * rows, rows), rows)


def rest_kernel(fsdp, cuts, high, own_gate, *refs):
    own_up, theirs = refs[: len(cuts)], refs[len(cuts): -5]
    out_gate, out_up, made, own_sem, write_sem = refs[-5:]
    columns, rows = own_gate.shape
    tile = min(columns, TILE)
    mine = column_of(0, fsdp, rows)

    copies = [pltpu.make_async_copy(own_gate, out_gate.at[:, mine], own_sem.at[0])]
    for k, (block, cut) in enumerate(zip(own_up, cuts)):
        copies.append(pltpu.make_async_copy(
            block.at[pl.ds(0, cut)], out_up.at[pl.ds(sum(cuts[:k]), cut), mine], own_sem.at[k + 1]
        ))
    for copy in copies:
        copy.start()
    for step in range(1, fsdp):
        weight, low = theirs[2 * step - 2: 2 * step]
        for j in range(columns // tile):
            piece = pl.ds(j * tile, tile)
            made[step - 1, piece] = merge(weight[:, piece], low[...], high[:, piece])
            copies.append(pltpu.make_async_copy(
                made.at[step - 1, piece], out_gate.at[piece, column_of(step, fsdp, rows)],
                write_sem.at[step - 1, j],
            ))
            copies[-1].start()
    for copy in copies:
        copy.wait()


def rest(fsdp, cuts, high, own_gate, own_up, theirs):
    columns, rows = own_gate.shape
    full = jax.ShapeDtypeStruct((columns, rows * fsdp), jnp.bfloat16)
    dma = pltpu.SemaphoreType.DMA
    operands = [high, own_gate, *own_up, *theirs]
    return pl.pallas_call(
        functools.partial(rest_kernel, fsdp, cuts),
        out_shape=[full, full],
        in_specs=[VMEM] * len(operands),
        out_specs=[ANY, ANY],
        scratch_shapes=[
            pltpu.VMEM((fsdp - 1, columns, rows), jnp.bfloat16),
            dma((1 + len(own_up),)), dma((fsdp - 1, columns // min(columns, TILE))),
        ],
        compiler_params=pltpu.CompilerParams(vmem_limit_bytes=12 * MIB),
        cost_estimate=cost(2 * rows * columns * high.shape[0], 6 * rows * columns),
    )(*[in_vmem(a) for a in operands])


def place_blocks(fsdp, start, cut, blocks, out, sem):
    copies = []
    for step, block in enumerate(blocks, 1):
        copies.append(pltpu.make_async_copy(
            block.at[pl.ds(0, cut)],
            out.at[pl.ds(start, cut), column_of(step, fsdp, block.shape[1])], sem.at[step - 1],
        ))
        copies[-1].start()
    return copies


def first_kernel(sizes, cut, norm_all, *refs):
    fsdp, model = sizes
    blocks, (_, out, serve_norm, gain, sem) = refs[:-5], refs[-5:]
    copies = place_blocks(fsdp, 0, cut, blocks, out, sem)
    gain[...] = norm_all[0] + norm_all[1]
    size = gain.shape[-1]
    for step, block in enumerate(blocks, 1):
        source = lax.rem(lax.axis_index("fsdp") + (fsdp - step), fsdp)
        piece = block[cut:, :size].astype(jnp.float32)[:1]
        gain[source * model + lax.axis_index("model")] = piece
    for k in range(gain.shape[0]):
        serve_norm[pl.ds(k * size, size)] = gain[k, 0, :].astype(serve_norm.dtype)
    for copy in copies:
        copy.wait()


def place_kernel(fsdp, start, cut, *refs):
    blocks, (_, out, sem) = refs[:-3], refs[-3:]
    for copy in place_blocks(fsdp, start, cut, blocks, out, sem):
        copy.wait()


def place(sizes, start, cut, blocks, held, norm_all=None):
    fsdp, _ = sizes
    size = (fsdp - 1) * cut * blocks[0].shape[1]
    operands = [in_vmem(a) for a in ([] if norm_all is None else [norm_all]) + blocks]
    out_shape, scratch = [jax.ShapeDtypeStruct(held.shape, held.dtype)], []
    kernel = functools.partial(place_kernel, fsdp, start, cut)
    if norm_all is not None:
        out_shape.append(jax.ShapeDtypeStruct((norm_all[0].size,), jnp.bfloat16))
        scratch.append(pltpu.VMEM(norm_all.shape[1:], jnp.float32))
        kernel = functools.partial(first_kernel, sizes, cut)
    return pl.pallas_call(
        kernel,
        out_shape=out_shape,
        in_specs=[VMEM] * len(operands) + [ANY],
        out_specs=[ANY, VMEM][: len(out_shape)],
        scratch_shapes=scratch + [pltpu.SemaphoreType.DMA((fsdp - 1,))],
        input_output_aliases={len(operands): 0},
        compiler_params=pltpu.CompilerParams(vmem_limit_bytes=MIB),
        cost_estimate=cost(32 * size, 2 * size),
    )(*operands, held)


def send(array, fsdp):
    return [
        lax.ppermute(array, "fsdp", [(i, (i + step) % fsdp) for i in range(fsdp)])
        for step in range(1, fsdp)
    ]


def body(sizes, weight_gate, low_gate, high_gate, weight_up, low_up, high_up, norm_train, norm_step):
    fsdp, _ = sizes
    low_gate, low_up = low_gate.T, low_up.T
    its_gate = send(in_hbm(weight_gate), fsdp)
    its_low = send(in_hbm(low_gate), fsdp)
    columns = weight_up.shape[1]
    cuts = tuple(columns * share // 4 for share in SHARES)
    groups = [(weight_gate, low_gate, high_gate), (weight_up, low_up, high_up)]
    norms = [norm_train.reshape(1, -1), norm_step.reshape(1, -1)]
    norm_all, own_gate, *own_up = own_part(sizes, cuts, groups, norms)
    its_up = [send(a, fsdp) for a in own_up]
    theirs = [a for pair in zip(its_gate, its_low) for a in pair]
    gate, up = rest(fsdp, cuts, high_gate, own_gate, own_up, theirs)
    up, serve_norm = place(sizes, 0, cuts[0], its_up[0], up, norm_all)
    for k in range(1, len(cuts)):
        up, = place(sizes, sum(cuts[:k]), cuts[k], its_up[k], up)
    return gate, up, serve_norm


def solution(mesh):
    whole = P(("ens", "fsdp", "model"))
    rows, thin, high = P(("ens", "fsdp"), "model"), P(("ens", "fsdp"), None), P("ens", "model")
    return jax.shard_map(
        functools.partial(body, (mesh.shape["fsdp"], mesh.shape["model"])),
        mesh=mesh,
        in_specs=(rows, thin, high, rows, thin, high, whole, whole),
        out_specs=(P(("ens", "model"), None), P(("ens", "model"), None), P("ens")),
        check_vma=False,
    )
```

```python
import functools

import jax
import jax.numpy as jnp
from jax import lax
from jax.experimental import pallas as pl
from jax.experimental.pallas import tpu as pltpu
from jax.sharding import PartitionSpec as P


mix_rate = 2.0
MIB = 2 ** 20
MESH = pl.DeviceIdType.MESH
VMEM, HBM = pl.BlockSpec(memory_space=pltpu.VMEM), pl.BlockSpec(memory_space=pltpu.HBM)
ANY = pl.BlockSpec(memory_space=pl.ANY)

TILE = 256
CUTS = ((2, 2), (1, 1, 2))
IN_FLIGHT = 3
EXTRA = 16


def in_vmem(array):
    return pltpu.with_memory_space_constraint(array, pltpu.VMEM)


def in_hbm(array):
    return pltpu.with_memory_space_constraint(array, pltpu.HBM)


def merge(weight, low, high):
    product = lax.dot_general(
        high, low * mix_rate, (((0,), (0,)), ((), ())), preferred_element_type=jnp.float32
    )
    return (weight.T.astype(jnp.float32) + product).astype(jnp.bfloat16)


def cost(flops, size):
    return pl.CostEstimate(flops=flops, bytes_accessed=size, transcendentals=0)


def blocks_of(rows):
    order = []
    for i in (1, 0):
        start = 0
        for cut in CUTS[i] if rows % 512 == 0 else (4,):
            order.append((i, start, rows * cut // 4))
            start += rows * cut // 4
    return order


def own_kernel(sizes, *refs):
    fsdp, model = sizes
    ins, norms, (norm_all, pack, *outs) = refs[:6], refs[6:8], refs[8:12]
    held, low_held, high_held, read_sem, small_sem, keep_sem, send_sem, recv_sem = refs[12:]
    rows, columns = ins[0].shape
    row, column = lax.axis_index("fsdp"), lax.axis_index("model")
    barrier = pltpu.get_barrier_semaphore()

    def peer(shift):
        return {
            "fsdp": lax.rem(row + shift // (model - 1), fsdp),
            "model": lax.rem(column + 1 + shift % (model - 1), model),
        }

    peers = range(fsdp * (model - 1))
    for shift in peers:
        pl.semaphore_signal(barrier, inc=1, device_id=peer(shift), device_id_type=MESH)

    place = row * model + column
    keep = [
        pltpu.make_async_copy(norms[i], norm_all.at[i, place], keep_sem.at[i]) for i in range(2)
    ]
    smalls = [
        [
            pltpu.make_async_copy(ins[3 * i + 1], low_held.at[i], small_sem.at[i, 0]),
            pltpu.make_async_copy(ins[3 * i + 2], high_held.at[i], small_sem.at[i, 1]),
        ]
        for i in range(2)
    ]
    order = blocks_of(rows)
    reads = [
        pltpu.make_async_copy(
            ins[3 * i].at[pl.ds(start, size)], held.at[i, pl.ds(start, size)], read_sem.at[n]
        )
        for n, (i, start, size) in enumerate(order)
    ]
    for copy in smalls[1] + reads[:IN_FLIGHT] + keep + smalls[0]:
        copy.start()

    def pieces():
        return [
            pltpu.make_async_remote_copy(
                src_ref=norm_all.at[k, place], dst_ref=norm_all.at[k, place],
                send_sem=send_sem.at[k, shift], recv_sem=recv_sem.at[k, shift],
                device_id=peer(shift), device_id_type=MESH,
            )
            for shift in peers for k in range(2)
        ]

    moment = jnp.minimum(jnp.maximum(3 - 4 * column // model, 1), len(order))

    def exchange(n):
        @pl.when(moment == n)
        def _():
            pl.semaphore_wait(barrier, len(peers))
            for copy in pieces():
                copy.start()

    for copy in keep:
        copy.wait()
    ahead = IN_FLIGHT
    ready = set()
    for n, (i, start, size) in enumerate(order):
        exchange(n)
        if i not in ready:
            for copy in smalls[i]:
                copy.wait()
            ready.add(i)
        reads[n].wait()
        if ahead < len(reads):
            reads[ahead].start()
            ahead += 1
        band = slice(start, start + size)
        for first in range(0, columns, min(columns, TILE)):
            piece = slice(first, first + min(columns, TILE))
            outs[i][piece, band] = merge(
                held[i, band, piece], low_held[i, :, band], high_held[i, :, piece]
            )
    exchange(len(order))
    rank, size = low_held.shape[1], norm_all.shape[-1]
    pack[:rank] = low_held[1]
    pack[rank:, :size] = jnp.broadcast_to(
        norm_all[0, place] + norm_all[1, place], (EXTRA, size)
    ).astype(pack.dtype)
    for copy in pieces():
        copy.wait()


def own_part(sizes, groups, norms):
    fsdp, model = sizes
    rows, columns = groups[0][0].shape
    rank = groups[0][1].shape[0]
    count, dma = fsdp * model, pltpu.SemaphoreType.DMA
    return pl.pallas_call(
        functools.partial(own_kernel, sizes),
        out_shape=[
            pltpu.VMEM((2, count) + norms[0].shape, jnp.float32),
            pltpu.VMEM((rank + EXTRA, rows), jnp.bfloat16),
            pltpu.VMEM((columns, rows), jnp.bfloat16),
            pltpu.VMEM((columns, rows), jnp.bfloat16),
        ],
        in_specs=[HBM] * 8,
        out_specs=[VMEM] * 4,
        scratch_shapes=[
            pltpu.VMEM((2, rows, columns), jnp.bfloat16),
            pltpu.VMEM((2, rank, rows), jnp.bfloat16),
            pltpu.VMEM((2, rank, columns), jnp.bfloat16),
            dma((len(blocks_of(rows)),)), dma((2, 2)), dma((2,)), dma((2, count)), dma((2, count)),
        ],
        compiler_params=pltpu.CompilerParams(
            collective_id=0, has_side_effects=True, vmem_limit_bytes=12 * MIB
        ),
        cost_estimate=cost(4 * rows * columns * rank, 4 * rows * columns),
    )(*[in_hbm(a) for group in groups for a in group], *[in_hbm(a) for a in norms])


def column_of(step, fsdp, rows):
    source = lax.rem(lax.axis_index("fsdp") + (fsdp - step), fsdp)
    return pl.ds(pl.multiple_of(source * rows, rows), rows)


def merge_theirs(fsdp, weights, lows, high, out, made, sem):
    copies = []
    rank = high.shape[0]
    for step, (weight, low) in enumerate(zip(weights, lows), 1):
        rows, columns = weight.shape
        tile = min(columns, TILE)
        for j in range(columns // tile):
            piece = pl.ds(j * tile, tile)
            made[step - 1, piece] = merge(weight[:, piece], low[:rank], high[:, piece])
            copies.append(pltpu.make_async_copy(
                made.at[step - 1, piece], out.at[piece, column_of(step, fsdp, rows)],
                sem.at[step - 1, j],
            ))
            copies[-1].start()
    return copies


def gate_kernel(fsdp, own_gate, own_up, high, *refs):
    theirs, (out_gate, out_up, made, own_sem, write_sem) = refs[:-5], refs[-5:]
    mine = column_of(0, fsdp, own_gate.shape[1])
    copies = [
        pltpu.make_async_copy(own_gate, out_gate.at[:, mine], own_sem.at[0]),
        pltpu.make_async_copy(own_up, out_up.at[:, mine], own_sem.at[1]),
    ]
    for copy in copies:
        copy.start()
    copies += merge_theirs(fsdp, theirs[::2], theirs[1::2], high, out_gate, made, write_sem)
    for copy in copies:
        copy.wait()


def up_kernel(sizes, norm_all, high, *refs):
    fsdp, model = sizes
    theirs, (_, out, serve_norm, made, gain, held_norm, norm_sem, write_sem) = refs[:-8], refs[-8:]
    rank, size = high.shape[0], gain.shape[-1]
    gain[...] = norm_all[0] + norm_all[1]
    for step in range(1, fsdp):
        source = lax.rem(lax.axis_index("fsdp") + (fsdp - step), fsdp)
        piece = theirs[2 * step - 1][rank:, :size].astype(jnp.float32)[:1]
        gain[source * model + lax.axis_index("model")] = piece
    for k in range(gain.shape[0]):
        held_norm[pl.ds(k * size, size)] = gain[k, 0, :].astype(held_norm.dtype)
    copies = [pltpu.make_async_copy(held_norm, serve_norm, norm_sem)]
    copies[0].start()
    copies += merge_theirs(fsdp, theirs[::2], theirs[1::2], high, out, made, write_sem)
    for copy in copies:
        copy.wait()


def theirs_scratch(fsdp, columns, rows):
    return [
        pltpu.VMEM((fsdp - 1, columns, rows), jnp.bfloat16),
        pltpu.SemaphoreType.DMA((fsdp - 1, columns // min(columns, TILE))),
    ]


def gate_part(fsdp, own_gate, own_up, high, theirs):
    columns, rows = own_gate.shape
    full = jax.ShapeDtypeStruct((columns, rows * fsdp), jnp.bfloat16)
    operands = [own_gate, own_up, high, *theirs]
    made, sem = theirs_scratch(fsdp, columns, rows)
    return pl.pallas_call(
        functools.partial(gate_kernel, fsdp),
        out_shape=[full, full],
        in_specs=[VMEM] * len(operands),
        out_specs=[ANY, ANY],
        scratch_shapes=[made, pltpu.SemaphoreType.DMA((2,)), sem],
        compiler_params=pltpu.CompilerParams(vmem_limit_bytes=12 * MIB),
        cost_estimate=cost(2 * rows * columns * high.shape[0], 6 * rows * columns),
    )(*[in_vmem(a) for a in operands])


def up_part(sizes, norm_all, high, theirs, held):
    rows, columns = theirs[0].shape
    operands = [norm_all, high, *theirs]
    made, sem = theirs_scratch(sizes[0], columns, rows)
    return pl.pallas_call(
        functools.partial(up_kernel, sizes),
        out_shape=[
            jax.ShapeDtypeStruct(held.shape, held.dtype),
            jax.ShapeDtypeStruct((norm_all[0].size,), jnp.bfloat16),
        ],
        in_specs=[VMEM] * len(operands) + [ANY],
        out_specs=[ANY, HBM],
        scratch_shapes=[
            made, pltpu.VMEM(norm_all.shape[1:], jnp.float32),
            pltpu.VMEM((norm_all[0].size,), jnp.bfloat16), pltpu.SemaphoreType.DMA, sem,
        ],
        input_output_aliases={len(operands): 0},
        compiler_params=pltpu.CompilerParams(vmem_limit_bytes=12 * MIB),
        cost_estimate=cost(2 * rows * columns * high.shape[0], 2 * rows * columns),
    )(*[in_vmem(a) for a in operands], held)


def send(array, fsdp):
    return [
        lax.ppermute(array, "fsdp", [(i, (i + step) % fsdp) for i in range(fsdp)])
        for step in range(1, fsdp)
    ]


def paired(*lists):
    return [a for group in zip(*lists) for a in group]


def body(sizes, weight_gate, low_gate, high_gate, weight_up, low_up, high_up, norm_train, norm_step):
    fsdp, _ = sizes
    low_gate, low_up = low_gate.T, low_up.T
    its_gate = send(in_hbm(weight_gate), fsdp)
    its_low = send(in_hbm(low_gate), fsdp)
    its_up = send(in_hbm(weight_up), fsdp)
    groups = [(weight_gate, low_gate, high_gate), (weight_up, low_up, high_up)]
    norms = [norm_train.reshape(1, -1), norm_step.reshape(1, -1)]
    norm_all, pack, own_gate, own_up = own_part(sizes, groups, norms)
    its_pack = send(pack, fsdp)
    gate, up = gate_part(fsdp, own_gate, own_up, high_gate, paired(its_gate, its_low))
    up, serve_norm = up_part(sizes, norm_all, high_up, paired(its_up, its_pack), up)
    return gate, up, serve_norm


def solution(mesh):
    whole = P(("ens", "fsdp", "model"))
    rows, thin, high = P(("ens", "fsdp"), "model"), P(("ens", "fsdp"), None), P("ens", "model")
    return jax.shard_map(
        functools.partial(body, (mesh.shape["fsdp"], mesh.shape["model"])),
        mesh=mesh,
        in_specs=(rows, thin, high, rows, thin, high, whole, whole),
        out_specs=(P(("ens", "model"), None), P(("ens", "model"), None), P("ens")),
        check_vma=False,
    )
```

```python
import functools

import jax
import jax.numpy as jnp
from jax import lax
from jax.experimental import pallas as pl
from jax.experimental.pallas import tpu as pltpu
from jax.sharding import PartitionSpec as P


mix_rate = 2.0
MIB = 2 ** 20
MESH = pl.DeviceIdType.MESH
VMEM, HBM = pl.BlockSpec(memory_space=pltpu.VMEM), pl.BlockSpec(memory_space=pltpu.HBM)
ANY = pl.BlockSpec(memory_space=pl.ANY)

TILE = 256
CUTS = ((2, 2), (1, 1, 2))
IN_FLIGHT = 3
EXTRA = 16


def in_vmem(array):
    return pltpu.with_memory_space_constraint(array, pltpu.VMEM)


def in_hbm(array):
    return pltpu.with_memory_space_constraint(array, pltpu.HBM)


def merge(weight, low, high):
    product = lax.dot_general(
        high, low * mix_rate, (((0,), (0,)), ((), ())), preferred_element_type=jnp.float32
    )
    return (weight.T.astype(jnp.float32) + product).astype(jnp.bfloat16)


def cost(flops, size):
    return pl.CostEstimate(flops=flops, bytes_accessed=size, transcendentals=0)


def blocks_of(rows):
    order = []
    for i in (1, 0):
        start = 0
        for cut in CUTS[i] if rows % 512 == 0 else (4,):
            order.append((i, start, rows * cut // 4))
            start += rows * cut // 4
    return order


def own_kernel(sizes, *refs):
    _, model = sizes
    ins, norms, (norm_all, pack, *outs) = refs[:6], refs[6:8], refs[8:12]
    held, low_held, high_held, read_sem, small_sem, keep_sem, send_sem, recv_sem = refs[12:]
    rows, columns = ins[0].shape
    column = lax.axis_index("model")
    barrier = pltpu.get_barrier_semaphore()

    def peer(shift):
        return {"model": lax.rem(column + shift, model)}

    peers = range(1, model)
    for shift in peers:
        pl.semaphore_signal(barrier, inc=1, device_id=peer(shift), device_id_type=MESH)

    keep = [
        pltpu.make_async_copy(norms[i], norm_all.at[i, column], keep_sem.at[i]) for i in range(2)
    ]
    smalls = [
        [
            pltpu.make_async_copy(ins[3 * i + 1], low_held.at[i], small_sem.at[i, 0]),
            pltpu.make_async_copy(ins[3 * i + 2], high_held.at[i], small_sem.at[i, 1]),
        ]
        for i in range(2)
    ]
    order = blocks_of(rows)
    reads = [
        pltpu.make_async_copy(
            ins[3 * i].at[pl.ds(start, size)], held.at[i, pl.ds(start, size)], read_sem.at[n]
        )
        for n, (i, start, size) in enumerate(order)
    ]
    for copy in smalls[1] + reads[:IN_FLIGHT] + keep + smalls[0]:
        copy.start()

    def pieces():
        return [
            pltpu.make_async_remote_copy(
                src_ref=norm_all.at[k, column], dst_ref=norm_all.at[k, column],
                send_sem=send_sem.at[k, shift], recv_sem=recv_sem.at[k, shift],
                device_id=peer(shift), device_id_type=MESH,
            )
            for shift in peers for k in range(2)
        ]

    moment = jnp.minimum(jnp.maximum(3 - 6 * column // model, 0), len(order))

    def exchange(n):
        @pl.when(moment == n)
        def _():
            pl.semaphore_wait(barrier, len(peers))
            for copy in pieces():
                copy.start()

    for copy in keep:
        copy.wait()
    ahead = IN_FLIGHT
    ready = set()
    for n, (i, start, size) in enumerate(order):
        exchange(n)
        if i not in ready:
            for copy in smalls[i]:
                copy.wait()
            ready.add(i)
        reads[n].wait()
        if ahead < len(reads):
            reads[ahead].start()
            ahead += 1
        band = slice(start, start + size)
        for first in range(0, columns, min(columns, TILE)):
            piece = slice(first, first + min(columns, TILE))
            outs[i][piece, band] = merge(
                held[i, band, piece], low_held[i, :, band], high_held[i, :, piece]
            )
    exchange(len(order))
    for copy in pieces():
        copy.wait()
    rank, size = low_held.shape[1], norm_all.shape[-1]
    pack[:rank] = low_held[1]
    rows_of = [norm_all[0, k] + norm_all[1, k] for k in range(model)]
    rows_of += [rows_of[-1]] * (pack.shape[0] - rank - model)
    pack[rank:, :size] = jnp.concatenate(rows_of, axis=0).astype(pack.dtype)


def own_part(sizes, groups, norms):
    _, model = sizes
    rows, columns = groups[0][0].shape
    rank = groups[0][1].shape[0]
    extra, dma = -(-model // EXTRA) * EXTRA, pltpu.SemaphoreType.DMA
    return pl.pallas_call(
        functools.partial(own_kernel, sizes),
        out_shape=[
            pltpu.VMEM((2, model) + norms[0].shape, jnp.float32),
            pltpu.VMEM((rank + extra, rows), jnp.bfloat16),
            pltpu.VMEM((columns, rows), jnp.bfloat16),
            pltpu.VMEM((columns, rows), jnp.bfloat16),
        ],
        in_specs=[HBM] * 8,
        out_specs=[VMEM] * 4,
        scratch_shapes=[
            pltpu.VMEM((2, rows, columns), jnp.bfloat16),
            pltpu.VMEM((2, rank, rows), jnp.bfloat16),
            pltpu.VMEM((2, rank, columns), jnp.bfloat16),
            dma((len(blocks_of(rows)),)), dma((2, 2)), dma((2,)), dma((2, model)), dma((2, model)),
        ],
        compiler_params=pltpu.CompilerParams(
            collective_id=0, has_side_effects=True, vmem_limit_bytes=12 * MIB
        ),
        cost_estimate=cost(4 * rows * columns * rank, 4 * rows * columns),
    )(*[in_hbm(a) for group in groups for a in group], *[in_hbm(a) for a in norms])


def column_of(step, fsdp, rows):
    source = lax.rem(lax.axis_index("fsdp") + (fsdp - step), fsdp)
    return pl.ds(pl.multiple_of(source * rows, rows), rows)


def merge_theirs(fsdp, weights, lows, high, out, made, sem):
    copies = []
    rank = high.shape[0]
    for step, (weight, low) in enumerate(zip(weights, lows), 1):
        rows, columns = weight.shape
        tile = min(columns, TILE)
        for j in range(columns // tile):
            piece = pl.ds(j * tile, tile)
            made[step - 1, piece] = merge(weight[:, piece], low[:rank], high[:, piece])
            copies.append(pltpu.make_async_copy(
                made.at[step - 1, piece], out.at[piece, column_of(step, fsdp, rows)],
                sem.at[step - 1, j],
            ))
            copies[-1].start()
    return copies


def gate_kernel(fsdp, own_gate, own_up, high, *refs):
    theirs, (out_gate, out_up, made, own_sem, write_sem) = refs[:-5], refs[-5:]
    mine = column_of(0, fsdp, own_gate.shape[1])
    copies = [
        pltpu.make_async_copy(own_gate, out_gate.at[:, mine], own_sem.at[0]),
        pltpu.make_async_copy(own_up, out_up.at[:, mine], own_sem.at[1]),
    ]
    for copy in copies:
        copy.start()
    copies += merge_theirs(fsdp, theirs[::2], theirs[1::2], high, out_gate, made, write_sem)
    for copy in copies:
        copy.wait()


def up_kernel(sizes, norm_all, high, *refs):
    fsdp, model = sizes
    theirs, (_, out, serve_norm, made, gain, held_norm, norm_sem, write_sem) = refs[:-8], refs[-8:]
    rank, size = high.shape[0], gain.shape[-1]
    row = lax.axis_index("fsdp")
    for k in range(model):
        gain[row * model + k] = norm_all[0, k] + norm_all[1, k]
    for step in range(1, fsdp):
        source = lax.rem(row + (fsdp - step), fsdp)
        pieces = theirs[2 * step - 1][rank:, :size].astype(jnp.float32)
        for k in range(model):
            gain[source * model + k] = pieces[k: k + 1]
    for k in range(fsdp * model):
        held_norm[pl.ds(k * size, size)] = gain[k, 0, :].astype(held_norm.dtype)
    copies = [pltpu.make_async_copy(held_norm, serve_norm, norm_sem)]
    copies[0].start()
    copies += merge_theirs(fsdp, theirs[::2], theirs[1::2], high, out, made, write_sem)
    for copy in copies:
        copy.wait()


def theirs_scratch(fsdp, columns, rows):
    return [
        pltpu.VMEM((fsdp - 1, columns, rows), jnp.bfloat16),
        pltpu.SemaphoreType.DMA((fsdp - 1, columns // min(columns, TILE))),
    ]


def gate_part(fsdp, own_gate, own_up, high, theirs):
    columns, rows = own_gate.shape
    full = jax.ShapeDtypeStruct((columns, rows * fsdp), jnp.bfloat16)
    operands = [own_gate, own_up, high, *theirs]
    made, sem = theirs_scratch(fsdp, columns, rows)
    return pl.pallas_call(
        functools.partial(gate_kernel, fsdp),
        out_shape=[full, full],
        in_specs=[VMEM] * len(operands),
        out_specs=[ANY, ANY],
        scratch_shapes=[made, pltpu.SemaphoreType.DMA((2,)), sem],
        compiler_params=pltpu.CompilerParams(vmem_limit_bytes=12 * MIB),
        cost_estimate=cost(2 * rows * columns * high.shape[0], 6 * rows * columns),
    )(*[in_vmem(a) for a in operands])


def up_part(sizes, norm_all, high, theirs, held):
    rows, columns = theirs[0].shape
    operands = [norm_all, high, *theirs]
    count = sizes[0] * sizes[1]
    norm = jax.ShapeDtypeStruct((count * norm_all.shape[-1],), jnp.bfloat16)
    made, sem = theirs_scratch(sizes[0], columns, rows)
    return pl.pallas_call(
        functools.partial(up_kernel, sizes),
        out_shape=[
            jax.ShapeDtypeStruct(held.shape, held.dtype),
            norm,
        ],
        in_specs=[VMEM] * len(operands) + [ANY],
        out_specs=[ANY, HBM],
        scratch_shapes=[
            made, pltpu.VMEM((count,) + norm_all.shape[2:], jnp.float32),
            pltpu.VMEM(norm.shape, norm.dtype), pltpu.SemaphoreType.DMA, sem,
        ],
        input_output_aliases={len(operands): 0},
        compiler_params=pltpu.CompilerParams(vmem_limit_bytes=12 * MIB),
        cost_estimate=cost(2 * rows * columns * high.shape[0], 2 * rows * columns),
    )(*[in_vmem(a) for a in operands], held)


def send(array, fsdp):
    return [
        lax.ppermute(array, "fsdp", [(i, (i + step) % fsdp) for i in range(fsdp)])
        for step in range(1, fsdp)
    ]


def paired(*lists):
    return [a for group in zip(*lists) for a in group]


def body(sizes, weight_gate, low_gate, high_gate, weight_up, low_up, high_up, norm_train, norm_step):
    fsdp, _ = sizes
    low_gate, low_up = low_gate.T, low_up.T
    its_gate = send(in_hbm(weight_gate), fsdp)
    its_low = send(in_hbm(low_gate), fsdp)
    its_up = send(in_hbm(weight_up), fsdp)
    groups = [(weight_gate, low_gate, high_gate), (weight_up, low_up, high_up)]
    norms = [norm_train.reshape(1, -1), norm_step.reshape(1, -1)]
    norm_all, pack, own_gate, own_up = own_part(sizes, groups, norms)
    its_pack = send(pack, fsdp)
    gate, up = gate_part(fsdp, own_gate, own_up, high_gate, paired(its_gate, its_low))
    up, serve_norm = up_part(sizes, norm_all, high_up, paired(its_up, its_pack), up)
    return gate, up, serve_norm


def solution(mesh):
    whole = P(("ens", "fsdp", "model"))
    rows, thin, high = P(("ens", "fsdp"), "model"), P(("ens", "fsdp"), None), P("ens", "model")
    return jax.shard_map(
        functools.partial(body, (mesh.shape["fsdp"], mesh.shape["model"])),
        mesh=mesh,
        in_specs=(rows, thin, high, rows, thin, high, whole, whole),
        out_specs=(P(("ens", "model"), None), P(("ens", "model"), None), P("ens")),
        check_vma=False,
    )
```

```python
import functools

import jax
import jax.numpy as jnp
from jax import lax
from jax.experimental import pallas as pl
from jax.experimental.pallas import tpu as pltpu
from jax.sharding import PartitionSpec as P


mix_rate = 2.0
MIB = 2 ** 20
MESH = pl.DeviceIdType.MESH
VMEM, HBM = pl.BlockSpec(memory_space=pltpu.VMEM), pl.BlockSpec(memory_space=pltpu.HBM)
ANY = pl.BlockSpec(memory_space=pl.ANY)

TILE = 256
CUTS = ((2, 2), (1, 1, 2))
IN_FLIGHT = 3
SHARES = (3, 1)
EXTRA = 16


def in_vmem(array):
    return pltpu.with_memory_space_constraint(array, pltpu.VMEM)


def in_hbm(array):
    return pltpu.with_memory_space_constraint(array, pltpu.HBM)


def merge(weight, low, high):
    product = lax.dot_general(
        high, low * mix_rate, (((0,), (0,)), ((), ())), preferred_element_type=jnp.float32
    )
    return (weight.T.astype(jnp.float32) + product).astype(jnp.bfloat16)


def cost(flops, size):
    return pl.CostEstimate(flops=flops, bytes_accessed=size, transcendentals=0)


def blocks_of(rows):
    order = []
    for i in (1, 0):
        start = 0
        for cut in CUTS[i] if rows % 512 == 0 else (4,):
            order.append((i, start, rows * cut // 4))
            start += rows * cut // 4
    return order


def own_kernel(sizes, cuts, *refs):
    fsdp, model = sizes
    ins, norms, (norm_all, own_gate, *own_up) = refs[:6], refs[6:8], refs[8: 10 + len(cuts)]
    held, low_held, high_held, read_sem, small_sem, keep_sem, send_sem, recv_sem = refs[
        10 + len(cuts):
    ]
    rows, columns = ins[0].shape
    row, column = lax.axis_index("fsdp"), lax.axis_index("model")
    barrier = pltpu.get_barrier_semaphore()

    last = row == fsdp - 1

    def peer(shift, core=fsdp - 1):
        return {"fsdp": core, "model": lax.rem(column + shift, model)}

    peers = range(1, model)

    @pl.when(last)
    def _():
        for shift in peers:
            for core in range(fsdp):
                pl.semaphore_signal(
                    barrier, inc=1, device_id=peer(shift, core), device_id_type=MESH
                )

    place = row * model + column
    keep = [
        pltpu.make_async_copy(norms[i], norm_all.at[i, place], keep_sem.at[i]) for i in range(2)
    ]
    smalls = [
        [
            pltpu.make_async_copy(ins[3 * i + 1], low_held.at[i], small_sem.at[i, 0]),
            pltpu.make_async_copy(ins[3 * i + 2], high_held.at[i], small_sem.at[i, 1]),
        ]
        for i in range(2)
    ]
    order = blocks_of(rows)
    reads = [
        pltpu.make_async_copy(
            ins[3 * i].at[pl.ds(start, size)], held.at[i, pl.ds(start, size)], read_sem.at[n]
        )
        for n, (i, start, size) in enumerate(order)
    ]
    for copy in smalls[1] + reads[:IN_FLIGHT] + keep + smalls[0]:
        copy.start()

    def norm_copy(k, shift, core):
        here = core * model + column
        return pltpu.make_async_remote_copy(
            src_ref=norm_all.at[k, here], dst_ref=norm_all.at[k, here],
            send_sem=send_sem.at[k, shift], recv_sem=recv_sem.at[k, shift, core],
            device_id=peer(shift), device_id_type=MESH,
        )

    moment = jnp.minimum(jnp.maximum(3 - 6 * column // model, 0), len(order))

    def exchange(n):
        @pl.when(moment == n)
        def _():
            pl.semaphore_wait(barrier, len(peers))
            for shift in peers:
                for k in range(2):
                    norm_copy(k, shift, row).start()

    for copy in keep:
        copy.wait()
    ahead = IN_FLIGHT
    ready = set()
    for n, (i, start, size) in enumerate(order):
        exchange(n)
        if i not in ready:
            for copy in smalls[i]:
                copy.wait()
            ready.add(i)
        reads[n].wait()
        if ahead < len(reads):
            reads[ahead].start()
            ahead += 1
        band = slice(start, start + size)
        first = 0
        for k, size in enumerate(cuts if i else [columns]):
            out, tile = (own_up[k] if i else own_gate), min(size, TILE)
            for within in range(0, size, tile):
                piece = slice(first, first + tile)
                out[within: within + tile, band] = merge(
                    held[i, band, piece], low_held[i, :, band], high_held[i, :, piece]
                )
                first += tile
    exchange(len(order))
    for shift in peers:
        for k in range(2):
            norm_copy(k, shift, row).wait_send()

    @pl.when(last)
    def _():
        for shift in peers:
            for core in range(fsdp):
                for k in range(2):
                    norm_copy(k, shift, core).wait_recv()

    size = norm_all.shape[-1]
    lines = [norm_all[0, k] + norm_all[1, k] for k in (place, *range(fsdp * model))]
    lines += lines[:1] * (own_up[0].shape[0] - cuts[0] - len(lines))
    own_up[0][cuts[0]:, :size] = jnp.concatenate(lines, axis=0).astype(jnp.bfloat16)


def own_part(sizes, cuts, groups, norms):
    fsdp, model = sizes
    rows, columns = groups[0][0].shape
    rank = groups[0][1].shape[0]
    count, dma = fsdp * model, pltpu.SemaphoreType.DMA
    extra = -(-(1 + count) // EXTRA) * EXTRA
    return pl.pallas_call(
        functools.partial(own_kernel, sizes, cuts),
        out_shape=[
            pltpu.VMEM((2, count) + norms[0].shape, jnp.float32),
        ] + [
            pltpu.VMEM((cut, rows), jnp.bfloat16)
            for cut in (columns, cuts[0] + extra) + cuts[1:]
        ],
        in_specs=[HBM] * 8,
        out_specs=[VMEM] * (2 + len(cuts)),
        scratch_shapes=[
            pltpu.VMEM((2, rows, columns), jnp.bfloat16),
            pltpu.VMEM((2, rank, rows), jnp.bfloat16),
            pltpu.VMEM((2, rank, columns), jnp.bfloat16),
            dma((len(blocks_of(rows)),)), dma((2, 2)), dma((2,)), dma((2, model)), dma((2, model, fsdp)),
        ],
        compiler_params=pltpu.CompilerParams(
            collective_id=0, has_side_effects=True, vmem_limit_bytes=12 * MIB
        ),
        cost_estimate=cost(4 * rows * columns * rank, 4 * rows * columns),
    )(*[in_hbm(a) for group in groups for a in group], *[in_hbm(a) for a in norms])


def column_of(step, fsdp, rows):
    source = lax.rem(lax.axis_index("fsdp") + (fsdp - step), fsdp)
    return pl.ds(pl.multiple_of(source * rows, rows), rows)


def rest_kernel(fsdp, cuts, high, own_gate, *refs):
    own_up, theirs = refs[: len(cuts)], refs[len(cuts): -5]
    out_gate, out_up, made, own_sem, write_sem = refs[-5:]
    columns, rows = own_gate.shape
    tile = min(columns, TILE)
    mine = column_of(0, fsdp, rows)

    copies = [pltpu.make_async_copy(own_gate, out_gate.at[:, mine], own_sem.at[0])]
    for k, (block, cut) in enumerate(zip(own_up, cuts)):
        copies.append(pltpu.make_async_copy(
            block.at[pl.ds(0, cut)], out_up.at[pl.ds(sum(cuts[:k]), cut), mine], own_sem.at[k + 1]
        ))
    for copy in copies:
        copy.start()
    for step in range(1, fsdp):
        weight, low = theirs[2 * step - 2: 2 * step]
        for j in range(columns // tile):
            piece = pl.ds(j * tile, tile)
            made[step - 1, piece] = merge(weight[:, piece], low[...], high[:, piece])
            copies.append(pltpu.make_async_copy(
                made.at[step - 1, piece], out_gate.at[piece, column_of(step, fsdp, rows)],
                write_sem.at[step - 1, j],
            ))
            copies[-1].start()
    for copy in copies:
        copy.wait()


def rest(fsdp, cuts, high, own_gate, own_up, theirs):
    columns, rows = own_gate.shape
    full = jax.ShapeDtypeStruct((columns, rows * fsdp), jnp.bfloat16)
    dma = pltpu.SemaphoreType.DMA
    operands = [high, own_gate, *own_up, *theirs]
    return pl.pallas_call(
        functools.partial(rest_kernel, fsdp, cuts),
        out_shape=[full, full],
        in_specs=[VMEM] * len(operands),
        out_specs=[ANY, ANY],
        scratch_shapes=[
            pltpu.VMEM((fsdp - 1, columns, rows), jnp.bfloat16),
            dma((1 + len(own_up),)), dma((fsdp - 1, columns // min(columns, TILE))),
        ],
        compiler_params=pltpu.CompilerParams(vmem_limit_bytes=12 * MIB),
        cost_estimate=cost(2 * rows * columns * high.shape[0], 6 * rows * columns),
    )(*[in_vmem(a) for a in operands])


def place_blocks(fsdp, start, cut, blocks, out, sem):
    copies = []
    for step, block in enumerate(blocks, 1):
        copies.append(pltpu.make_async_copy(
            block.at[pl.ds(0, cut)],
            out.at[pl.ds(start, cut), column_of(step, fsdp, block.shape[1])], sem.at[step - 1],
        ))
        copies[-1].start()
    return copies


def first_kernel(sizes, cut, norm_all, *refs):
    fsdp, model = sizes
    blocks, (_, out, serve_norm, gain, held_norm, norm_sem, sem) = refs[:-7], refs[-7:]
    copies = place_blocks(fsdp, 0, cut, blocks, out, sem)
    size = gain.shape[-1]
    row, column = lax.axis_index("fsdp"), lax.axis_index("model")
    sources = [lax.rem(row + (fsdp - step), fsdp) for step in range(1, fsdp)]
    lines = [block[cut:, :size].astype(jnp.float32) for block in blocks]
    for k in range(fsdp * model):
        value = norm_all[0, k] + norm_all[1, k]
        for source, line in zip(sources, lines):
            value = jnp.where(source == fsdp - 1, line[k + 1: k + 2], value)
        gain[k] = value
    place = row * model + column
    gain[place] = norm_all[0, place] + norm_all[1, place]
    for source, line in zip(sources, lines):
        gain[source * model + column] = line[:1]
    for k in range(fsdp * model):
        held_norm[pl.ds(k * size, size)] = gain[k, 0, :].astype(held_norm.dtype)
    copies.append(pltpu.make_async_copy(held_norm, serve_norm, norm_sem))
    copies[-1].start()
    for copy in copies:
        copy.wait()


def place_kernel(fsdp, start, cut, *refs):
    blocks, (_, out, sem) = refs[:-3], refs[-3:]
    for copy in place_blocks(fsdp, start, cut, blocks, out, sem):
        copy.wait()


def place(sizes, start, cut, blocks, held, norm_all=None):
    fsdp, _ = sizes
    size = (fsdp - 1) * cut * blocks[0].shape[1]
    operands = [in_vmem(a) for a in ([] if norm_all is None else [norm_all]) + blocks]
    out_shape, scratch = [jax.ShapeDtypeStruct(held.shape, held.dtype)], []
    kernel = functools.partial(place_kernel, fsdp, start, cut)
    if norm_all is not None:
        out_shape.append(jax.ShapeDtypeStruct((norm_all[0].size,), jnp.bfloat16))
        scratch += [
            pltpu.VMEM(norm_all.shape[1:], jnp.float32),
            pltpu.VMEM((norm_all[0].size,), jnp.bfloat16), pltpu.SemaphoreType.DMA,
        ]
        kernel = functools.partial(first_kernel, sizes, cut)
    return pl.pallas_call(
        kernel,
        out_shape=out_shape,
        in_specs=[VMEM] * len(operands) + [ANY],
        out_specs=[ANY, HBM][: len(out_shape)],
        scratch_shapes=scratch + [pltpu.SemaphoreType.DMA((fsdp - 1,))],
        input_output_aliases={len(operands): 0},
        compiler_params=pltpu.CompilerParams(vmem_limit_bytes=MIB),
        cost_estimate=cost(32 * size, 2 * size),
    )(*operands, held)


def send(array, fsdp):
    return [
        lax.ppermute(array, "fsdp", [(i, (i + step) % fsdp) for i in range(fsdp)])
        for step in range(1, fsdp)
    ]


def body(sizes, weight_gate, low_gate, high_gate, weight_up, low_up, high_up, norm_train, norm_step):
    fsdp, _ = sizes
    low_gate, low_up = low_gate.T, low_up.T
    its_gate = send(in_hbm(weight_gate), fsdp)
    its_low = send(in_hbm(low_gate), fsdp)
    columns = weight_up.shape[1]
    cuts = tuple(columns * share // 4 for share in SHARES)
    groups = [(weight_gate, low_gate, high_gate), (weight_up, low_up, high_up)]
    norms = [norm_train.reshape(1, -1), norm_step.reshape(1, -1)]
    norm_all, own_gate, *own_up = own_part(sizes, cuts, groups, norms)
    its_up = [send(a, fsdp) for a in own_up]
    theirs = [a for pair in zip(its_gate, its_low) for a in pair]
    gate, up = rest(fsdp, cuts, high_gate, own_gate, own_up, theirs)
    up, serve_norm = place(sizes, 0, cuts[0], its_up[0], up, norm_all)
    for k in range(1, len(cuts)):
        up, = place(sizes, sum(cuts[:k]), cuts[k], its_up[k], up)
    return gate, up, serve_norm


def solution(mesh):
    whole = P(("ens", "fsdp", "model"))
    rows, thin, high = P(("ens", "fsdp"), "model"), P(("ens", "fsdp"), None), P("ens", "model")
    return jax.shard_map(
        functools.partial(body, (mesh.shape["fsdp"], mesh.shape["model"])),
        mesh=mesh,
        in_specs=(rows, thin, high, rows, thin, high, whole, whole),
        out_specs=(P(("ens", "model"), None), P(("ens", "model"), None), P("ens")),
        check_vma=False,
    )
```

```python
import functools

import jax
import jax.numpy as jnp
from jax import lax
from jax.experimental import pallas as pl
from jax.experimental.pallas import tpu as pltpu
from jax.sharding import PartitionSpec as P


mix_rate = 2.0
MIB = 2 ** 20
MESH = pl.DeviceIdType.MESH
VMEM, HBM = pl.BlockSpec(memory_space=pltpu.VMEM), pl.BlockSpec(memory_space=pltpu.HBM)
ANY = pl.BlockSpec(memory_space=pl.ANY)

TILE = 256
CUTS = ((2, 2), (1, 1, 2))
IN_FLIGHT = 3
EXTRA = 16


def in_vmem(array):
    return pltpu.with_memory_space_constraint(array, pltpu.VMEM)


def in_hbm(array):
    return pltpu.with_memory_space_constraint(array, pltpu.HBM)


def merge(weight, low, high):
    product = lax.dot_general(
        high, low * mix_rate, (((0,), (0,)), ((), ())), preferred_element_type=jnp.float32
    )
    return (weight.T.astype(jnp.float32) + product).astype(jnp.bfloat16)


def cost(flops, size):
    return pl.CostEstimate(flops=flops, bytes_accessed=size, transcendentals=0)


def blocks_of(rows):
    order = []
    for i in (1, 0):
        start = 0
        for cut in CUTS[i] if rows % 512 == 0 else (4,):
            order.append((i, start, rows * cut // 4))
            start += rows * cut // 4
    return order


def own_kernel(sizes, *refs):
    _, model = sizes
    ins, norms, (norm_all, pack, *outs) = refs[:6], refs[6:8], refs[8:12]
    held, low_held, high_held, read_sem, small_sem, keep_sem, send_sem, recv_sem = refs[12:]
    rows, columns = ins[0].shape
    column = lax.axis_index("model")
    barrier = pltpu.get_barrier_semaphore()

    def peer(shift):
        return {"model": lax.rem(column + shift, model)}

    peers = range(1, model)
    for shift in peers:
        pl.semaphore_signal(barrier, inc=1, device_id=peer(shift), device_id_type=MESH)

    keep = [
        pltpu.make_async_copy(norms[i], norm_all.at[i, column], keep_sem.at[i]) for i in range(2)
    ]
    smalls = [
        [
            pltpu.make_async_copy(ins[3 * i + 1], low_held.at[i], small_sem.at[i, 0]),
            pltpu.make_async_copy(ins[3 * i + 2], high_held.at[i], small_sem.at[i, 1]),
        ]
        for i in range(2)
    ]
    order = blocks_of(rows)
    reads = [
        pltpu.make_async_copy(
            ins[3 * i].at[pl.ds(start, size)], held.at[i, pl.ds(start, size)], read_sem.at[n]
        )
        for n, (i, start, size) in enumerate(order)
    ]
    for copy in smalls[1] + reads[:IN_FLIGHT] + keep + smalls[0]:
        copy.start()

    def pieces():
        return [
            pltpu.make_async_remote_copy(
                src_ref=norm_all.at[k, column], dst_ref=norm_all.at[k, column],
                send_sem=send_sem.at[k, shift], recv_sem=recv_sem.at[k, shift],
                device_id=peer(shift), device_id_type=MESH,
            )
            for shift in peers for k in range(2)
        ]

    moment = jnp.minimum(jnp.maximum(3 - 6 * column // model, 0), len(order))

    def exchange(n):
        @pl.when(moment == n)
        def _():
            pl.semaphore_wait(barrier, len(peers))
            for copy in pieces():
                copy.start()

    for copy in keep:
        copy.wait()
    ahead = IN_FLIGHT
    ready = set()
    for n, (i, start, size) in enumerate(order):
        exchange(n)
        if i not in ready:
            for copy in smalls[i]:
                copy.wait()
            ready.add(i)
        reads[n].wait()
        if ahead < len(reads):
            reads[ahead].start()
            ahead += 1
        band = slice(start, start + size)
        for first in range(0, columns, min(columns, TILE)):
            piece = slice(first, first + min(columns, TILE))
            outs[i][piece, band] = merge(
                held[i, band, piece], low_held[i, :, band], high_held[i, :, piece]
            )
    exchange(len(order))
    for copy in pieces():
        copy.wait()
    rank, size = low_held.shape[1], norm_all.shape[-1]
    pack[:rank] = low_held[1]
    rows_of = [norm_all[0, k] + norm_all[1, k] for k in range(model)]
    rows_of += [rows_of[-1]] * (pack.shape[0] - rank - model)
    pack[rank:, :size] = jnp.concatenate(rows_of, axis=0).astype(pack.dtype)


def own_part(sizes, groups, norms):
    _, model = sizes
    rows, columns = groups[0][0].shape
    rank = groups[0][1].shape[0]
    extra, dma = -(-model // EXTRA) * EXTRA, pltpu.SemaphoreType.DMA
    return pl.pallas_call(
        functools.partial(own_kernel, sizes),
        out_shape=[
            pltpu.VMEM((2, model) + norms[0].shape, jnp.float32),
            pltpu.VMEM((rank + extra, rows), jnp.bfloat16),
            pltpu.VMEM((columns, rows), jnp.bfloat16),
            pltpu.VMEM((columns, rows), jnp.bfloat16),
        ],
        in_specs=[HBM] * 8,
        out_specs=[VMEM] * 4,
        scratch_shapes=[
            pltpu.VMEM((2, rows, columns), jnp.bfloat16),
            pltpu.VMEM((2, rank, rows), jnp.bfloat16),
            pltpu.VMEM((2, rank, columns), jnp.bfloat16),
            dma((len(blocks_of(rows)),)), dma((2, 2)), dma((2,)), dma((2, model)), dma((2, model)),
        ],
        compiler_params=pltpu.CompilerParams(
            collective_id=0, has_side_effects=True, vmem_limit_bytes=12 * MIB
        ),
        cost_estimate=cost(4 * rows * columns * rank, 4 * rows * columns),
    )(*[in_hbm(a) for group in groups for a in group], *[in_hbm(a) for a in norms])


def column_of(step, fsdp, rows):
    source = lax.rem(lax.axis_index("fsdp") + (fsdp - step), fsdp)
    return pl.ds(pl.multiple_of(source * rows, rows), rows)


def merge_theirs(fsdp, weights, lows, high, out, made, sem):
    copies = []
    rank = high.shape[0]
    for step, (weight, low) in enumerate(zip(weights, lows), 1):
        rows, columns = weight.shape
        tile = min(columns, TILE)
        for j in range(columns // tile):
            piece = pl.ds(j * tile, tile)
            made[step - 1, piece] = merge(weight[:, piece], low[:rank], high[:, piece])
            copies.append(pltpu.make_async_copy(
                made.at[step - 1, piece], out.at[piece, column_of(step, fsdp, rows)],
                sem.at[step - 1, j],
            ))
            copies[-1].start()
    return copies


def first_chip():
    return lax.axis_index("ens") + lax.axis_index("model") == 0


def early_kernel(weight, low, high, out, held, low_held, high_held, made, sem, write_sem):
    rows, columns = weight.shape
    part, tile = held.shape[0], min(columns, TILE)
    column = pl.multiple_of(lax.axis_index("fsdp") * rows, part)

    @pl.when(first_chip())
    def _():
        reads = [
            pltpu.make_async_copy(low, low_held, sem.at[0]),
            pltpu.make_async_copy(high, high_held, sem.at[1]),
            pltpu.make_async_copy(weight.at[pl.ds(0, part)], held, sem.at[2]),
        ]
        for copy in reads:
            copy.start()
        for copy in reads:
            copy.wait()
        writes = []
        for j in range(columns // tile):
            piece = pl.ds(j * tile, tile)
            made[piece] = merge(held[:, piece], low_held[:, :part], high_held[:, piece])
            writes.append(pltpu.make_async_copy(
                made.at[piece], out.at[piece, pl.ds(column, part)], write_sem.at[j]
            ))
            writes[-1].start()
        for copy in writes:
            copy.wait()


def early_part(fsdp, weight, low, high):
    rows, columns = weight.shape
    rank, part = low.shape[0], rows // 2 if rows % 256 == 0 else rows
    dma = pltpu.SemaphoreType.DMA
    return pl.pallas_call(
        early_kernel,
        out_shape=jax.ShapeDtypeStruct((columns, rows * fsdp), jnp.bfloat16),
        in_specs=[HBM] * 3,
        out_specs=ANY,
        scratch_shapes=[
            pltpu.VMEM((part, columns), jnp.bfloat16),
            pltpu.VMEM((rank, rows), jnp.bfloat16),
            pltpu.VMEM((rank, columns), jnp.bfloat16),
            pltpu.VMEM((columns, part), jnp.bfloat16),
            dma((3,)), dma((columns // min(columns, TILE),)),
        ],
        compiler_params=pltpu.CompilerParams(vmem_limit_bytes=12 * MIB),
        cost_estimate=cost(rows * columns * rank, rows * columns),
    )(*[in_hbm(a) for a in (weight, low, high)])


def gate_kernel(fsdp, own_gate, own_up, high, *refs):
    theirs, (_, out_gate, out_up, made, own_sem, write_sem) = refs[:-6], refs[-6:]
    rows = own_gate.shape[1]
    part = rows // 2 if rows % 256 == 0 else rows
    mine = column_of(0, fsdp, rows)
    copies = [pltpu.make_async_copy(own_gate, out_gate.at[:, mine], own_sem.at[0])]
    if part < rows:
        second = pl.ds(pl.multiple_of(lax.axis_index("fsdp") * rows + part, part), rows - part)
        copies.append(pltpu.make_async_copy(
            own_up.at[:, pl.ds(part, rows - part)], out_up.at[:, second], own_sem.at[1]
        ))
    first = pl.ds(pl.multiple_of(lax.axis_index("fsdp") * rows, part), part)
    unwritten = pltpu.make_async_copy(
        own_up.at[:, pl.ds(0, part)], out_up.at[:, first], own_sem.at[2]
    )
    for copy in copies:
        copy.start()
    pl.when(jnp.logical_not(first_chip()))(unwritten.start)
    copies += merge_theirs(fsdp, theirs[::2], theirs[1::2], high, out_gate, made, write_sem)
    for copy in copies:
        copy.wait()
    pl.when(jnp.logical_not(first_chip()))(unwritten.wait)


def up_kernel(sizes, norm_all, high, *refs):
    fsdp, model = sizes
    theirs, (_, out, serve_norm, made, gain, held_norm, norm_sem, write_sem) = refs[:-8], refs[-8:]
    rank, size = high.shape[0], gain.shape[-1]
    row = lax.axis_index("fsdp")
    for k in range(model):
        gain[row * model + k] = norm_all[0, k] + norm_all[1, k]
    for step in range(1, fsdp):
        source = lax.rem(row + (fsdp - step), fsdp)
        pieces = theirs[2 * step - 1][rank:, :size].astype(jnp.float32)
        for k in range(model):
            gain[source * model + k] = pieces[k: k + 1]
    for k in range(fsdp * model):
        held_norm[pl.ds(k * size, size)] = gain[k, 0, :].astype(held_norm.dtype)
    copies = [pltpu.make_async_copy(held_norm, serve_norm, norm_sem)]
    copies[0].start()
    copies += merge_theirs(fsdp, theirs[::2], theirs[1::2], high, out, made, write_sem)
    for copy in copies:
        copy.wait()


def theirs_scratch(fsdp, columns, rows):
    return [
        pltpu.VMEM((fsdp - 1, columns, rows), jnp.bfloat16),
        pltpu.SemaphoreType.DMA((fsdp - 1, columns // min(columns, TILE))),
    ]


def gate_part(fsdp, own_gate, own_up, high, theirs, held):
    columns, rows = own_gate.shape
    full = jax.ShapeDtypeStruct((columns, rows * fsdp), jnp.bfloat16)
    operands = [own_gate, own_up, high, *theirs]
    made, sem = theirs_scratch(fsdp, columns, rows)
    return pl.pallas_call(
        functools.partial(gate_kernel, fsdp),
        out_shape=[full, full],
        in_specs=[VMEM] * len(operands) + [ANY],
        out_specs=[ANY, ANY],
        scratch_shapes=[made, pltpu.SemaphoreType.DMA((3,)), sem],
        input_output_aliases={len(operands): 1},
        compiler_params=pltpu.CompilerParams(vmem_limit_bytes=12 * MIB),
        cost_estimate=cost(2 * rows * columns * high.shape[0], 6 * rows * columns),
    )(*[in_vmem(a) for a in operands], held)


def up_part(sizes, norm_all, high, theirs, held):
    rows, columns = theirs[0].shape
    operands = [norm_all, high, *theirs]
    count = sizes[0] * sizes[1]
    norm = jax.ShapeDtypeStruct((count * norm_all.shape[-1],), jnp.bfloat16)
    made, sem = theirs_scratch(sizes[0], columns, rows)
    return pl.pallas_call(
        functools.partial(up_kernel, sizes),
        out_shape=[
            jax.ShapeDtypeStruct(held.shape, held.dtype),
            norm,
        ],
        in_specs=[VMEM] * len(operands) + [ANY],
        out_specs=[ANY, HBM],
        scratch_shapes=[
            made, pltpu.VMEM((count,) + norm_all.shape[2:], jnp.float32),
            pltpu.VMEM(norm.shape, norm.dtype), pltpu.SemaphoreType.DMA, sem,
        ],
        input_output_aliases={len(operands): 0},
        compiler_params=pltpu.CompilerParams(vmem_limit_bytes=12 * MIB),
        cost_estimate=cost(2 * rows * columns * high.shape[0], 2 * rows * columns),
    )(*[in_vmem(a) for a in operands], held)


def send(array, fsdp):
    return [
        lax.ppermute(array, "fsdp", [(i, (i + step) % fsdp) for i in range(fsdp)])
        for step in range(1, fsdp)
    ]


def paired(*lists):
    return [a for group in zip(*lists) for a in group]


def body(sizes, weight_gate, low_gate, high_gate, weight_up, low_up, high_up, norm_train, norm_step):
    fsdp, _ = sizes
    low_gate, low_up = low_gate.T, low_up.T
    its_gate = send(in_hbm(weight_gate), fsdp)
    its_low = send(in_hbm(low_gate), fsdp)
    its_up = send(in_hbm(weight_up), fsdp)
    groups = [(weight_gate, low_gate, high_gate), (weight_up, low_up, high_up)]
    up = early_part(fsdp, weight_up, low_up, high_up)
    norm_train, norm_step, up = lax.optimization_barrier((norm_train, norm_step, up))
    norms = [norm_train.reshape(1, -1), norm_step.reshape(1, -1)]
    norm_all, pack, own_gate, own_up = own_part(sizes, groups, norms)
    its_pack = send(pack, fsdp)
    gate, up = gate_part(fsdp, own_gate, own_up, high_gate, paired(its_gate, its_low), up)
    up, serve_norm = up_part(sizes, norm_all, high_up, paired(its_up, its_pack), up)
    return gate, up, serve_norm


def solution(mesh):
    whole = P(("ens", "fsdp", "model"))
    rows, thin, high = P(("ens", "fsdp"), "model"), P(("ens", "fsdp"), None), P("ens", "model")
    return jax.shard_map(
        functools.partial(body, (mesh.shape["fsdp"], mesh.shape["model"])),
        mesh=mesh,
        in_specs=(rows, thin, high, rows, thin, high, whole, whole),
        out_specs=(P(("ens", "model"), None), P(("ens", "model"), None), P("ens")),
        check_vma=False,
    )
```

```python
import functools

import jax
import jax.numpy as jnp
from jax import lax
from jax.experimental import pallas as pl
from jax.experimental.pallas import tpu as pltpu
from jax.sharding import PartitionSpec as P


mix_rate = 2.0
MIB = 2 ** 20
MESH = pl.DeviceIdType.MESH
VMEM, HBM = pl.BlockSpec(memory_space=pltpu.VMEM), pl.BlockSpec(memory_space=pltpu.HBM)
ANY = pl.BlockSpec(memory_space=pl.ANY)

TILE = 256
CUTS = ((2, 2), (1, 1, 2))
IN_FLIGHT = 3
EXTRA = 16


def in_vmem(array):
    return pltpu.with_memory_space_constraint(array, pltpu.VMEM)


def in_hbm(array):
    return pltpu.with_memory_space_constraint(array, pltpu.HBM)


def merge(weight, low, high):
    product = lax.dot_general(
        high, low * mix_rate, (((0,), (0,)), ((), ())), preferred_element_type=jnp.float32
    )
    return (weight.T.astype(jnp.float32) + product).astype(jnp.bfloat16)


def cost(flops, size):
    return pl.CostEstimate(flops=flops, bytes_accessed=size, transcendentals=0)


def first_chip():
    return lax.axis_index("ens") + lax.axis_index("model") == 0


def early_rows(rows):
    return rows // 2 if rows % 512 == 0 else rows


def blocks_of(rows):
    order = []
    for i in (1, 0):
        start = 0
        for cut in CUTS[i] if rows % 512 == 0 else (4,):
            order.append((i, start, rows * cut // 4))
            start += rows * cut // 4
    return order


def own_kernel(sizes, *refs):
    _, model = sizes
    ins, norms, (norm_all, pack, *outs) = refs[:6], refs[6:8], refs[8:12]
    held, low_held, high_held, read_sem, small_sem, keep_sem, send_sem, recv_sem = refs[12:]
    rows, columns = ins[0].shape
    column = lax.axis_index("model")
    barrier = pltpu.get_barrier_semaphore()

    def peer(shift):
        return {"model": lax.rem(column + shift, model)}

    peers = range(1, model)
    for shift in peers:
        pl.semaphore_signal(barrier, inc=1, device_id=peer(shift), device_id_type=MESH)

    keep = [
        pltpu.make_async_copy(norms[i], norm_all.at[i, column], keep_sem.at[i]) for i in range(2)
    ]
    smalls = [
        [
            pltpu.make_async_copy(ins[3 * i + 1], low_held.at[i], small_sem.at[i, 0]),
            pltpu.make_async_copy(ins[3 * i + 2], high_held.at[i], small_sem.at[i, 1]),
        ]
        for i in range(2)
    ]
    order = blocks_of(rows)
    reads = [
        pltpu.make_async_copy(
            ins[3 * i].at[pl.ds(start, size)], held.at[i, pl.ds(start, size)], read_sem.at[n]
        )
        for n, (i, start, size) in enumerate(order)
    ]
    for copy in smalls[1] + reads[:IN_FLIGHT] + keep + smalls[0]:
        copy.start()

    def pieces():
        return [
            pltpu.make_async_remote_copy(
                src_ref=norm_all.at[k, column], dst_ref=norm_all.at[k, column],
                send_sem=send_sem.at[k, shift], recv_sem=recv_sem.at[k, shift],
                device_id=peer(shift), device_id_type=MESH,
            )
            for shift in peers for k in range(2)
        ]

    moment = jnp.minimum(jnp.maximum(3 - 6 * column // model, 0), len(order))

    def exchange(n):
        @pl.when(moment == n)
        def _():
            pl.semaphore_wait(barrier, len(peers))
            for copy in pieces():
                copy.start()

    for copy in keep:
        copy.wait()
    ahead = IN_FLIGHT
    ready = set()
    for n, (i, start, size) in enumerate(order):
        exchange(n)
        if i not in ready:
            for copy in smalls[i]:
                copy.wait()
            ready.add(i)
        reads[n].wait()
        if ahead < len(reads):
            reads[ahead].start()
            ahead += 1

        def merge_block(i=i, band=slice(start, start + size)):
            for first in range(0, columns, min(columns, TILE)):
                piece = slice(first, first + min(columns, TILE))
                outs[i][piece, band] = merge(
                    held[i, band, piece], low_held[i, :, band], high_held[i, :, piece]
                )

        if i == 1 and start + size <= early_rows(rows):
            pl.when(jnp.logical_not(first_chip()))(merge_block)
        else:
            merge_block()
    exchange(len(order))
    for copy in pieces():
        copy.wait()
    rank, size = low_held.shape[1], norm_all.shape[-1]
    pack[:rank] = low_held[1]
    rows_of = [norm_all[0, k] + norm_all[1, k] for k in range(model)]
    rows_of += [rows_of[-1]] * (pack.shape[0] - rank - model)
    pack[rank:, :size] = jnp.concatenate(rows_of, axis=0).astype(pack.dtype)


def own_part(sizes, groups, norms):
    _, model = sizes
    rows, columns = groups[0][0].shape
    rank = groups[0][1].shape[0]
    extra, dma = -(-model // EXTRA) * EXTRA, pltpu.SemaphoreType.DMA
    return pl.pallas_call(
        functools.partial(own_kernel, sizes),
        out_shape=[
            pltpu.VMEM((2, model) + norms[0].shape, jnp.float32),
            pltpu.VMEM((rank + extra, rows), jnp.bfloat16),
            pltpu.VMEM((columns, rows), jnp.bfloat16),
            pltpu.VMEM((columns, rows), jnp.bfloat16),
        ],
        in_specs=[HBM] * 8,
        out_specs=[VMEM] * 4,
        scratch_shapes=[
            pltpu.VMEM((2, rows, columns), jnp.bfloat16),
            pltpu.VMEM((2, rank, rows), jnp.bfloat16),
            pltpu.VMEM((2, rank, columns), jnp.bfloat16),
            dma((len(blocks_of(rows)),)), dma((2, 2)), dma((2,)), dma((2, model)), dma((2, model)),
        ],
        compiler_params=pltpu.CompilerParams(
            collective_id=0, has_side_effects=True, vmem_limit_bytes=12 * MIB
        ),
        cost_estimate=cost(4 * rows * columns * rank, 4 * rows * columns),
    )(*[in_hbm(a) for group in groups for a in group], *[in_hbm(a) for a in norms])


def column_of(step, fsdp, rows):
    source = lax.rem(lax.axis_index("fsdp") + (fsdp - step), fsdp)
    return pl.ds(pl.multiple_of(source * rows, rows), rows)


def merge_theirs(fsdp, weights, lows, high, out, made, sem):
    copies = []
    rank = high.shape[0]
    for step, (weight, low) in enumerate(zip(weights, lows), 1):
        rows, columns = weight.shape
        tile = min(columns, TILE)
        for j in range(columns // tile):
            piece = pl.ds(j * tile, tile)
            made[step - 1, piece] = merge(weight[:, piece], low[:rank], high[:, piece])
            copies.append(pltpu.make_async_copy(
                made.at[step - 1, piece], out.at[piece, column_of(step, fsdp, rows)],
                sem.at[step - 1, j],
            ))
            copies[-1].start()
    return copies


def early_kernel(weight, low, high, out, held, low_held, high_held, made, sem, write_sem):
    rows, columns = weight.shape
    part, tile = held.shape[0], min(columns, TILE)
    column = pl.multiple_of(lax.axis_index("fsdp") * rows, rows)

    @pl.when(first_chip())
    def _():
        size = part // 2 if part % 256 == 0 else part
        bands = [slice(start, start + size) for start in range(0, part, size)]
        smalls = [
            pltpu.make_async_copy(low, low_held, sem.at[0]),
            pltpu.make_async_copy(high, high_held, sem.at[1]),
        ]
        reads = [
            pltpu.make_async_copy(
                weight.at[pl.ds(band.start, size)], held.at[pl.ds(band.start, size)],
                sem.at[2 + k],
            )
            for k, band in enumerate(bands)
        ]
        for copy in smalls + reads:
            copy.start()
        for copy in smalls:
            copy.wait()
        writes = []
        for k, band in enumerate(bands):
            reads[k].wait()
            for j in range(columns // tile):
                piece = pl.ds(j * tile, tile)
                made[piece, band] = merge(held[band, piece], low_held[:, band], high_held[:, piece])
            writes.append(pltpu.make_async_copy(
                made.at[:, pl.ds(band.start, size)],
                out.at[:, pl.ds(column + band.start, size)], write_sem.at[k],
            ))
            writes[-1].start()
        for copy in writes:
            copy.wait()


def early_part(fsdp, weight, low, high):
    rows, columns = weight.shape
    rank, part = low.shape[0], early_rows(rows)
    dma = pltpu.SemaphoreType.DMA
    return pl.pallas_call(
        early_kernel,
        out_shape=jax.ShapeDtypeStruct((columns, rows * fsdp), jnp.bfloat16),
        in_specs=[HBM] * 3,
        out_specs=ANY,
        scratch_shapes=[
            pltpu.VMEM((part, columns), jnp.bfloat16),
            pltpu.VMEM((rank, rows), jnp.bfloat16),
            pltpu.VMEM((rank, columns), jnp.bfloat16),
            pltpu.VMEM((columns, part), jnp.bfloat16),
            dma((4,)), dma((2,)),
        ],
        compiler_params=pltpu.CompilerParams(vmem_limit_bytes=12 * MIB),
        cost_estimate=cost(rows * columns * rank, rows * columns),
    )(*[in_hbm(a) for a in (weight, low, high)])


def gate_kernel(fsdp, own_gate, own_up, high, *refs):
    theirs, (_, out_gate, out_up, made, own_sem, write_sem) = refs[:-6], refs[-6:]
    rows = own_gate.shape[1]
    part = early_rows(rows)
    mine = column_of(0, fsdp, rows)
    copies = [pltpu.make_async_copy(own_gate, out_gate.at[:, mine], own_sem.at[0])]
    if part < rows:
        second = pl.ds(pl.multiple_of(lax.axis_index("fsdp") * rows + part, part), rows - part)
        copies.append(pltpu.make_async_copy(
            own_up.at[:, pl.ds(part, rows - part)], out_up.at[:, second], own_sem.at[1]
        ))
    first = pl.ds(pl.multiple_of(lax.axis_index("fsdp") * rows, part), part)
    unwritten = pltpu.make_async_copy(
        own_up.at[:, pl.ds(0, part)], out_up.at[:, first], own_sem.at[2]
    )
    for copy in copies:
        copy.start()
    pl.when(jnp.logical_not(first_chip()))(unwritten.start)
    copies += merge_theirs(fsdp, theirs[::2], theirs[1::2], high, out_gate, made, write_sem)
    for copy in copies:
        copy.wait()
    pl.when(jnp.logical_not(first_chip()))(unwritten.wait)


def up_kernel(sizes, norm_all, high, *refs):
    fsdp, model = sizes
    theirs, (_, out, serve_norm, made, gain, held_norm, norm_sem, write_sem) = refs[:-8], refs[-8:]
    rank, size = high.shape[0], gain.shape[-1]
    row = lax.axis_index("fsdp")
    for k in range(model):
        gain[row * model + k] = norm_all[0, k] + norm_all[1, k]
    for step in range(1, fsdp):
        source = lax.rem(row + (fsdp - step), fsdp)
        pieces = theirs[2 * step - 1][rank:, :size].astype(jnp.float32)
        for k in range(model):
            gain[source * model + k] = pieces[k: k + 1]
    for k in range(fsdp * model):
        held_norm[pl.ds(k * size, size)] = gain[k, 0, :].astype(held_norm.dtype)
    copies = [pltpu.make_async_copy(held_norm, serve_norm, norm_sem)]
    copies[0].start()
    copies += merge_theirs(fsdp, theirs[::2], theirs[1::2], high, out, made, write_sem)
    for copy in copies:
        copy.wait()


def theirs_scratch(fsdp, columns, rows):
    return [
        pltpu.VMEM((fsdp - 1, columns, rows), jnp.bfloat16),
        pltpu.SemaphoreType.DMA((fsdp - 1, columns // min(columns, TILE))),
    ]


def gate_part(fsdp, own_gate, own_up, high, theirs, held):
    columns, rows = own_gate.shape
    full = jax.ShapeDtypeStruct((columns, rows * fsdp), jnp.bfloat16)
    operands = [own_gate, own_up, high, *theirs]
    made, sem = theirs_scratch(fsdp, columns, rows)
    return pl.pallas_call(
        functools.partial(gate_kernel, fsdp),
        out_shape=[full, full],
        in_specs=[VMEM] * len(operands) + [ANY],
        out_specs=[ANY, ANY],
        scratch_shapes=[made, pltpu.SemaphoreType.DMA((3,)), sem],
        input_output_aliases={len(operands): 1},
        compiler_params=pltpu.CompilerParams(vmem_limit_bytes=12 * MIB),
        cost_estimate=cost(2 * rows * columns * high.shape[0], 6 * rows * columns),
    )(*[in_vmem(a) for a in operands], held)


def up_part(sizes, norm_all, high, theirs, held):
    rows, columns = theirs[0].shape
    operands = [norm_all, high, *theirs]
    count = sizes[0] * sizes[1]
    norm = jax.ShapeDtypeStruct((count * norm_all.shape[-1],), jnp.bfloat16)
    made, sem = theirs_scratch(sizes[0], columns, rows)
    return pl.pallas_call(
        functools.partial(up_kernel, sizes),
        out_shape=[
            jax.ShapeDtypeStruct(held.shape, held.dtype),
            norm,
        ],
        in_specs=[VMEM] * len(operands) + [ANY],
        out_specs=[ANY, HBM],
        scratch_shapes=[
            made, pltpu.VMEM((count,) + norm_all.shape[2:], jnp.float32),
            pltpu.VMEM(norm.shape, norm.dtype), pltpu.SemaphoreType.DMA, sem,
        ],
        input_output_aliases={len(operands): 0},
        compiler_params=pltpu.CompilerParams(vmem_limit_bytes=12 * MIB),
        cost_estimate=cost(2 * rows * columns * high.shape[0], 2 * rows * columns),
    )(*[in_vmem(a) for a in operands], held)


def send(array, fsdp):
    return [
        lax.ppermute(array, "fsdp", [(i, (i + step) % fsdp) for i in range(fsdp)])
        for step in range(1, fsdp)
    ]


def paired(*lists):
    return [a for group in zip(*lists) for a in group]


def body(sizes, weight_gate, low_gate, high_gate, weight_up, low_up, high_up, norm_train, norm_step):
    fsdp, _ = sizes
    low_gate, low_up = low_gate.T, low_up.T
    its_gate = send(in_hbm(weight_gate), fsdp)
    its_low = send(in_hbm(low_gate), fsdp)
    its_up = send(in_hbm(weight_up), fsdp)
    groups = [(weight_gate, low_gate, high_gate), (weight_up, low_up, high_up)]
    up = early_part(fsdp, weight_up, low_up, high_up)
    norm_train, norm_step, up = lax.optimization_barrier((norm_train, norm_step, up))
    norms = [norm_train.reshape(1, -1), norm_step.reshape(1, -1)]
    norm_all, pack, own_gate, own_up = own_part(sizes, groups, norms)
    its_pack = send(pack, fsdp)
    gate, up = gate_part(fsdp, own_gate, own_up, high_gate, paired(its_gate, its_low), up)
    up, serve_norm = up_part(sizes, norm_all, high_up, paired(its_up, its_pack), up)
    return gate, up, serve_norm


def solution(mesh):
    whole = P(("ens", "fsdp", "model"))
    rows, thin, high = P(("ens", "fsdp"), "model"), P(("ens", "fsdp"), None), P("ens", "model")
    return jax.shard_map(
        functools.partial(body, (mesh.shape["fsdp"], mesh.shape["model"])),
        mesh=mesh,
        in_specs=(rows, thin, high, rows, thin, high, whole, whole),
        out_specs=(P(("ens", "model"), None), P(("ens", "model"), None), P("ens")),
        check_vma=False,
    )
```

```python
import functools

import jax
import jax.numpy as jnp
from jax import lax
from jax.experimental import pallas as pl
from jax.experimental.pallas import tpu as pltpu
from jax.sharding import PartitionSpec as P


mix_rate = 2.0
MIB = 2 ** 20
MESH = pl.DeviceIdType.MESH
VMEM, HBM = pl.BlockSpec(memory_space=pltpu.VMEM), pl.BlockSpec(memory_space=pltpu.HBM)
ANY = pl.BlockSpec(memory_space=pl.ANY)

TILE = 256
CUTS = ((2, 2), (1, 1, 2))
IN_FLIGHT = 3
EXTRA = 16


def in_vmem(array):
    return pltpu.with_memory_space_constraint(array, pltpu.VMEM)


def in_hbm(array):
    return pltpu.with_memory_space_constraint(array, pltpu.HBM)


def merge(weight, low, high):
    product = lax.dot_general(
        high, low * mix_rate, (((0,), (0,)), ((), ())), preferred_element_type=jnp.float32
    )
    return (weight.T.astype(jnp.float32) + product).astype(jnp.bfloat16)


def cost(flops, size):
    return pl.CostEstimate(flops=flops, bytes_accessed=size, transcendentals=0)


def first_chip():
    return lax.axis_index("ens") + lax.axis_index("model") == 0


def early_rows(rows):
    return rows // 4 if rows % 512 == 0 else rows


def blocks_of(rows):
    order = []
    for i in (1, 0):
        start = 0
        for cut in CUTS[i] if rows % 512 == 0 else (4,):
            order.append((i, start, rows * cut // 4))
            start += rows * cut // 4
    return order


def own_kernel(sizes, *refs):
    _, model = sizes
    ins, norms, (norm_all, pack, *outs) = refs[:6], refs[6:8], refs[8:12]
    held, low_held, high_held, read_sem, small_sem, keep_sem, send_sem, recv_sem = refs[12:]
    rows, columns = ins[0].shape
    column = lax.axis_index("model")
    barrier = pltpu.get_barrier_semaphore()

    def peer(shift):
        return {"model": lax.rem(column + shift, model)}

    peers = range(1, model)
    for shift in peers:
        pl.semaphore_signal(barrier, inc=1, device_id=peer(shift), device_id_type=MESH)

    keep = [
        pltpu.make_async_copy(norms[i], norm_all.at[i, column], keep_sem.at[i]) for i in range(2)
    ]
    smalls = [
        [
            pltpu.make_async_copy(ins[3 * i + 1], low_held.at[i], small_sem.at[i, 0]),
            pltpu.make_async_copy(ins[3 * i + 2], high_held.at[i], small_sem.at[i, 1]),
        ]
        for i in range(2)
    ]
    order = blocks_of(rows)
    reads = [
        pltpu.make_async_copy(
            ins[3 * i].at[pl.ds(start, size)], held.at[i, pl.ds(start, size)], read_sem.at[n]
        )
        for n, (i, start, size) in enumerate(order)
    ]
    for copy in smalls[1] + reads[:IN_FLIGHT] + keep + smalls[0]:
        copy.start()

    def pieces():
        return [
            pltpu.make_async_remote_copy(
                src_ref=norm_all.at[k, column], dst_ref=norm_all.at[k, column],
                send_sem=send_sem.at[k, shift], recv_sem=recv_sem.at[k, shift],
                device_id=peer(shift), device_id_type=MESH,
            )
            for shift in peers for k in range(2)
        ]

    moment = jnp.minimum(jnp.maximum(3 - 6 * column // model, 0), len(order))

    def exchange(n):
        @pl.when(moment == n)
        def _():
            pl.semaphore_wait(barrier, len(peers))
            for copy in pieces():
                copy.start()

    for copy in keep:
        copy.wait()
    ahead = IN_FLIGHT
    ready = set()
    for n, (i, start, size) in enumerate(order):
        exchange(n)
        if i not in ready:
            for copy in smalls[i]:
                copy.wait()
            ready.add(i)
        reads[n].wait()
        if ahead < len(reads):
            reads[ahead].start()
            ahead += 1

        def merge_block(i=i, band=slice(start, start + size)):
            for first in range(0, columns, min(columns, TILE)):
                piece = slice(first, first + min(columns, TILE))
                outs[i][piece, band] = merge(
                    held[i, band, piece], low_held[i, :, band], high_held[i, :, piece]
                )

        if i == 1 and start + size <= early_rows(rows):
            pl.when(jnp.logical_not(first_chip()))(merge_block)
        else:
            merge_block()
    exchange(len(order))
    for copy in pieces():
        copy.wait()
    lines = [norm_all[0, k] + norm_all[1, k] for k in range(model)]
    lines += lines[-1:] * (pack.shape[0] - model)
    pack[...] = jnp.concatenate(lines, axis=0).astype(pack.dtype)


def own_part(sizes, groups, norms):
    _, model = sizes
    rows, columns = groups[0][0].shape
    rank = groups[0][1].shape[0]
    extra, dma = -(-model // EXTRA) * EXTRA, pltpu.SemaphoreType.DMA
    return pl.pallas_call(
        functools.partial(own_kernel, sizes),
        out_shape=[
            pltpu.VMEM((2, model) + norms[0].shape, jnp.float32),
            pltpu.VMEM((extra, norms[0].shape[1]), jnp.bfloat16),
            pltpu.VMEM((columns, rows), jnp.bfloat16),
            pltpu.VMEM((columns, rows), jnp.bfloat16),
        ],
        in_specs=[HBM] * 8,
        out_specs=[VMEM] * 4,
        scratch_shapes=[
            pltpu.VMEM((2, rows, columns), jnp.bfloat16),
            pltpu.VMEM((2, rank, rows), jnp.bfloat16),
            pltpu.VMEM((2, rank, columns), jnp.bfloat16),
            dma((len(blocks_of(rows)),)), dma((2, 2)), dma((2,)), dma((2, model)), dma((2, model)),
        ],
        compiler_params=pltpu.CompilerParams(
            collective_id=0, has_side_effects=True, vmem_limit_bytes=12 * MIB
        ),
        cost_estimate=cost(4 * rows * columns * rank, 4 * rows * columns),
    )(*[in_hbm(a) for group in groups for a in group], *[in_hbm(a) for a in norms])


def column_of(step, fsdp, rows):
    source = lax.rem(lax.axis_index("fsdp") + (fsdp - step), fsdp)
    return pl.ds(pl.multiple_of(source * rows, rows), rows)


def merge_theirs(fsdp, weights, lows, high, out, made, sem):
    copies = []
    for step, (weight, low) in enumerate(zip(weights, lows), 1):
        rows, columns = weight.shape
        tile = min(columns, TILE)
        for j in range(columns // tile):
            piece = pl.ds(j * tile, tile)
            made[step - 1, piece] = merge(weight[:, piece], low[...], high[:, piece])
            copies.append(pltpu.make_async_copy(
                made.at[step - 1, piece], out.at[piece, column_of(step, fsdp, rows)],
                sem.at[step - 1, j],
            ))
            copies[-1].start()
    return copies


def early_kernel(weight, low, high, out, held, low_held, high_held, made, sem, write_sem):
    rows, columns = weight.shape
    part, tile = held.shape[0], min(columns, TILE)
    column = pl.multiple_of(lax.axis_index("fsdp") * rows, rows)

    @pl.when(first_chip())
    def _():
        size = part // 2 if part % 512 == 0 else part
        bands = [slice(start, start + size) for start in range(0, part, size)]
        smalls = [
            pltpu.make_async_copy(low, low_held, sem.at[0]),
            pltpu.make_async_copy(high, high_held, sem.at[1]),
        ]
        reads = [
            pltpu.make_async_copy(
                weight.at[pl.ds(band.start, size)], held.at[pl.ds(band.start, size)],
                sem.at[2 + k],
            )
            for k, band in enumerate(bands)
        ]
        for copy in smalls + reads:
            copy.start()
        for copy in smalls:
            copy.wait()
        writes = []
        for k, band in enumerate(bands):
            reads[k].wait()
            for j in range(columns // tile):
                piece = pl.ds(j * tile, tile)
                made[piece, band] = merge(held[band, piece], low_held[:, band], high_held[:, piece])
            writes.append(pltpu.make_async_copy(
                made.at[:, pl.ds(band.start, size)],
                out.at[:, pl.ds(column + band.start, size)], write_sem.at[k],
            ))
            writes[-1].start()
        for copy in writes:
            copy.wait()


def early_part(fsdp, weight, low, high):
    rows, columns = weight.shape
    rank, part = low.shape[0], early_rows(rows)
    dma = pltpu.SemaphoreType.DMA
    return pl.pallas_call(
        early_kernel,
        out_shape=jax.ShapeDtypeStruct((columns, rows * fsdp), jnp.bfloat16),
        in_specs=[HBM] * 3,
        out_specs=ANY,
        scratch_shapes=[
            pltpu.VMEM((part, columns), jnp.bfloat16),
            pltpu.VMEM((rank, rows), jnp.bfloat16),
            pltpu.VMEM((rank, columns), jnp.bfloat16),
            pltpu.VMEM((columns, part), jnp.bfloat16),
            dma((4,)), dma((2,)),
        ],
        compiler_params=pltpu.CompilerParams(vmem_limit_bytes=12 * MIB),
        cost_estimate=cost(rows * columns * rank, rows * columns),
    )(*[in_hbm(a) for a in (weight, low, high)])


def gate_kernel(fsdp, own_gate, own_up, high, *refs):
    theirs, (_, out_gate, out_up, made, own_sem, write_sem) = refs[:-6], refs[-6:]
    rows = own_gate.shape[1]
    part = early_rows(rows)
    mine = column_of(0, fsdp, rows)
    copies = [pltpu.make_async_copy(own_gate, out_gate.at[:, mine], own_sem.at[0])]
    if part < rows:
        second = pl.ds(pl.multiple_of(lax.axis_index("fsdp") * rows + part, part), rows - part)
        copies.append(pltpu.make_async_copy(
            own_up.at[:, pl.ds(part, rows - part)], out_up.at[:, second], own_sem.at[1]
        ))
    first = pl.ds(pl.multiple_of(lax.axis_index("fsdp") * rows, part), part)
    unwritten = pltpu.make_async_copy(
        own_up.at[:, pl.ds(0, part)], out_up.at[:, first], own_sem.at[2]
    )
    for copy in copies:
        copy.start()
    pl.when(jnp.logical_not(first_chip()))(unwritten.start)
    copies += merge_theirs(fsdp, theirs[::2], theirs[1::2], high, out_gate, made, write_sem)
    for copy in copies:
        copy.wait()
    pl.when(jnp.logical_not(first_chip()))(unwritten.wait)


def up_kernel(sizes, norm_all, high, *refs):
    fsdp, model = sizes
    theirs, (_, out, serve_norm, made, gain, held_norm, norm_sem, write_sem) = refs[:-8], refs[-8:]
    size = gain.shape[-1]
    row = lax.axis_index("fsdp")
    for k in range(model):
        gain[row * model + k] = norm_all[0, k] + norm_all[1, k]
    for step in range(1, fsdp):
        source = lax.rem(row + (fsdp - step), fsdp)
        pieces = theirs[3 * step - 1][...].astype(jnp.float32)
        for k in range(model):
            gain[source * model + k] = pieces[k: k + 1]
    for k in range(fsdp * model):
        held_norm[pl.ds(k * size, size)] = gain[k, 0, :].astype(held_norm.dtype)
    copies = [pltpu.make_async_copy(held_norm, serve_norm, norm_sem)]
    copies[0].start()
    copies += merge_theirs(fsdp, theirs[::3], theirs[1::3], high, out, made, write_sem)
    for copy in copies:
        copy.wait()


def theirs_scratch(fsdp, columns, rows):
    return [
        pltpu.VMEM((fsdp - 1, columns, rows), jnp.bfloat16),
        pltpu.SemaphoreType.DMA((fsdp - 1, columns // min(columns, TILE))),
    ]


def gate_part(fsdp, own_gate, own_up, high, theirs, held):
    columns, rows = own_gate.shape
    full = jax.ShapeDtypeStruct((columns, rows * fsdp), jnp.bfloat16)
    operands = [own_gate, own_up, high, *theirs]
    made, sem = theirs_scratch(fsdp, columns, rows)
    return pl.pallas_call(
        functools.partial(gate_kernel, fsdp),
        out_shape=[full, full],
        in_specs=[VMEM] * len(operands) + [ANY],
        out_specs=[ANY, ANY],
        scratch_shapes=[made, pltpu.SemaphoreType.DMA((3,)), sem],
        input_output_aliases={len(operands): 1},
        compiler_params=pltpu.CompilerParams(vmem_limit_bytes=12 * MIB),
        cost_estimate=cost(2 * rows * columns * high.shape[0], 6 * rows * columns),
    )(*[in_vmem(a) for a in operands], held)


def up_part(sizes, norm_all, high, theirs, held):
    rows, columns = theirs[0].shape
    operands = [norm_all, high, *theirs]
    count = sizes[0] * sizes[1]
    norm = jax.ShapeDtypeStruct((count * norm_all.shape[-1],), jnp.bfloat16)
    made, sem = theirs_scratch(sizes[0], columns, rows)
    return pl.pallas_call(
        functools.partial(up_kernel, sizes),
        out_shape=[
            jax.ShapeDtypeStruct(held.shape, held.dtype),
            norm,
        ],
        in_specs=[VMEM] * len(operands) + [ANY],
        out_specs=[ANY, HBM],
        scratch_shapes=[
            made, pltpu.VMEM((count,) + norm_all.shape[2:], jnp.float32),
            pltpu.VMEM(norm.shape, norm.dtype), pltpu.SemaphoreType.DMA, sem,
        ],
        input_output_aliases={len(operands): 0},
        compiler_params=pltpu.CompilerParams(vmem_limit_bytes=12 * MIB),
        cost_estimate=cost(2 * rows * columns * high.shape[0], 2 * rows * columns),
    )(*[in_vmem(a) for a in operands], held)


def send(array, fsdp):
    return [
        lax.ppermute(array, "fsdp", [(i, (i + step) % fsdp) for i in range(fsdp)])
        for step in range(1, fsdp)
    ]


def paired(*lists):
    return [a for group in zip(*lists) for a in group]


def body(sizes, weight_gate, low_gate, high_gate, weight_up, low_up, high_up, norm_train, norm_step):
    fsdp, _ = sizes
    low_gate, low_up = low_gate.T, low_up.T
    its_gate = send(in_hbm(weight_gate), fsdp)
    its_low = send(in_hbm(low_gate), fsdp)
    its_low_up = send(in_hbm(low_up), fsdp)
    its_up = send(in_hbm(weight_up), fsdp)
    groups = [(weight_gate, low_gate, high_gate), (weight_up, low_up, high_up)]
    up = early_part(fsdp, weight_up, low_up, high_up)
    norm_train, norm_step, up = lax.optimization_barrier((norm_train, norm_step, up))
    norms = [norm_train.reshape(1, -1), norm_step.reshape(1, -1)]
    norm_all, pack, own_gate, own_up = own_part(sizes, groups, norms)
    its_pack = send(pack, fsdp)
    gate, up = gate_part(fsdp, own_gate, own_up, high_gate, paired(its_gate, its_low), up)
    up, serve_norm = up_part(sizes, norm_all, high_up, paired(its_up, its_low_up, its_pack), up)
    return gate, up, serve_norm


def solution(mesh):
    whole = P(("ens", "fsdp", "model"))
    rows, thin, high = P(("ens", "fsdp"), "model"), P(("ens", "fsdp"), None), P("ens", "model")
    return jax.shard_map(
        functools.partial(body, (mesh.shape["fsdp"], mesh.shape["model"])),
        mesh=mesh,
        in_specs=(rows, thin, high, rows, thin, high, whole, whole),
        out_specs=(P(("ens", "model"), None), P(("ens", "model"), None), P("ens")),
        check_vma=False,
    )
```

```python
import functools

import jax
import jax.numpy as jnp
from jax import lax
from jax.experimental import pallas as pl
from jax.experimental.pallas import tpu as pltpu
from jax.sharding import PartitionSpec as P


mix_rate = 2.0
MIB = 2 ** 20
MESH = pl.DeviceIdType.MESH
VMEM, HBM = pl.BlockSpec(memory_space=pltpu.VMEM), pl.BlockSpec(memory_space=pltpu.HBM)
ANY = pl.BlockSpec(memory_space=pl.ANY)

TILE = 256
CUTS = ((2, 2), (1, 1, 2))
IN_FLIGHT = 3
EXTRA = 16


def in_vmem(array):
    return pltpu.with_memory_space_constraint(array, pltpu.VMEM)


def in_hbm(array):
    return pltpu.with_memory_space_constraint(array, pltpu.HBM)


def merge(weight, low, high):
    product = lax.dot_general(
        high, low * mix_rate, (((0,), (0,)), ((), ())), preferred_element_type=jnp.float32
    )
    return (weight.T.astype(jnp.float32) + product).astype(jnp.bfloat16)


def cost(flops, size):
    return pl.CostEstimate(flops=flops, bytes_accessed=size, transcendentals=0)


def first_chip():
    return lax.axis_index("ens") + lax.axis_index("model") == 0


def early_rows(rows):
    return rows // 4 if rows % 512 == 0 else rows


def blocks_of(rows):
    order = []
    for i in (1, 0):
        start = 0
        for cut in CUTS[i] if rows % 512 == 0 else (4,):
            order.append((i, start, rows * cut // 4))
            start += rows * cut // 4
    return order


def own_kernel(sizes, *refs):
    _, model = sizes
    ins, norms, (norm_all, pack, *outs) = refs[:6], refs[6:8], refs[8:12]
    held, low_held, high_held, read_sem, small_sem, keep_sem, send_sem, recv_sem = refs[12:]
    rows, columns = ins[0].shape
    column = lax.axis_index("model")
    barrier = pltpu.get_barrier_semaphore()

    def peer(shift):
        return {"model": lax.rem(column + shift, model)}

    peers = range(1, model)
    for shift in peers:
        pl.semaphore_signal(barrier, inc=1, device_id=peer(shift), device_id_type=MESH)

    keep = [
        pltpu.make_async_copy(norms[i], norm_all.at[column, i], keep_sem.at[i]) for i in range(2)
    ]
    smalls = [
        [
            pltpu.make_async_copy(ins[3 * i + 1], low_held.at[i], small_sem.at[i, 0]),
            pltpu.make_async_copy(ins[3 * i + 2], high_held.at[i], small_sem.at[i, 1]),
        ]
        for i in range(2)
    ]
    order = blocks_of(rows)
    reads = [
        pltpu.make_async_copy(
            ins[3 * i].at[pl.ds(start, size)], held.at[i, pl.ds(start, size)], read_sem.at[n]
        )
        for n, (i, start, size) in enumerate(order)
    ]
    for copy in smalls[1] + reads[:IN_FLIGHT] + keep + smalls[0]:
        copy.start()

    def pieces():
        return [
            pltpu.make_async_remote_copy(
                src_ref=norm_all.at[column], dst_ref=norm_all.at[column],
                send_sem=send_sem.at[shift], recv_sem=recv_sem.at[shift],
                device_id=peer(shift), device_id_type=MESH,
            )
            for shift in peers
        ]

    moment = jnp.minimum(jnp.maximum(3 - 6 * column // model, 0), len(order))

    def exchange(n):
        @pl.when(moment == n)
        def _():
            pl.semaphore_wait(barrier, len(peers))
            for copy in pieces():
                copy.start()

    for copy in keep:
        copy.wait()
    ahead = IN_FLIGHT
    ready = set()
    for n, (i, start, size) in enumerate(order):
        exchange(n)
        if i not in ready:
            for copy in smalls[i]:
                copy.wait()
            ready.add(i)
        reads[n].wait()
        if ahead < len(reads):
            reads[ahead].start()
            ahead += 1

        def merge_block(i=i, band=slice(start, start + size)):
            for first in range(0, columns, min(columns, TILE)):
                piece = slice(first, first + min(columns, TILE))
                outs[i][piece, band] = merge(
                    held[i, band, piece], low_held[i, :, band], high_held[i, :, piece]
                )

        if i == 1 and start + size <= early_rows(rows):
            pl.when(jnp.logical_not(first_chip()))(merge_block)
        else:
            merge_block()
    exchange(len(order))
    for copy in pieces():
        copy.wait()
    rank, size = low_held.shape[1], norm_all.shape[-1]
    pack[:rank] = low_held[1]
    rows_of = [norm_all[k, 0] + norm_all[k, 1] for k in range(model)]
    rows_of += [rows_of[-1]] * (pack.shape[0] - rank - model)
    pack[rank:, :size] = jnp.concatenate(rows_of, axis=0).astype(pack.dtype)


def own_part(sizes, groups, norms):
    _, model = sizes
    rows, columns = groups[0][0].shape
    rank = groups[0][1].shape[0]
    extra, dma = -(-model // EXTRA) * EXTRA, pltpu.SemaphoreType.DMA
    return pl.pallas_call(
        functools.partial(own_kernel, sizes),
        out_shape=[
            pltpu.VMEM((model, 2) + norms[0].shape, jnp.float32),
            pltpu.VMEM((rank + extra, rows), jnp.bfloat16),
            pltpu.VMEM((columns, rows), jnp.bfloat16),
            pltpu.VMEM((columns, rows), jnp.bfloat16),
        ],
        in_specs=[HBM] * 8,
        out_specs=[VMEM] * 4,
        scratch_shapes=[
            pltpu.VMEM((2, rows, columns), jnp.bfloat16),
            pltpu.VMEM((2, rank, rows), jnp.bfloat16),
            pltpu.VMEM((2, rank, columns), jnp.bfloat16),
            dma((len(blocks_of(rows)),)), dma((2, 2)), dma((2,)), dma((model,)), dma((model,)),
        ],
        compiler_params=pltpu.CompilerParams(
            collective_id=0, has_side_effects=True, vmem_limit_bytes=12 * MIB
        ),
        cost_estimate=cost(4 * rows * columns * rank, 4 * rows * columns),
    )(*[in_hbm(a) for group in groups for a in group], *[in_hbm(a) for a in norms])


def column_of(step, fsdp, rows):
    source = lax.rem(lax.axis_index("fsdp") + (fsdp - step), fsdp)
    return pl.ds(pl.multiple_of(source * rows, rows), rows)


def merge_theirs(fsdp, weights, lows, high, out, made, sem):
    copies = []
    rank = high.shape[0]
    for step, (weight, low) in enumerate(zip(weights, lows), 1):
        rows, columns = weight.shape
        tile = min(columns, TILE)
        for j in range(columns // tile):
            piece = pl.ds(j * tile, tile)
            made[step - 1, piece] = merge(weight[:, piece], low[:rank], high[:, piece])
            copies.append(pltpu.make_async_copy(
                made.at[step - 1, piece], out.at[piece, column_of(step, fsdp, rows)],
                sem.at[step - 1, j],
            ))
            copies[-1].start()
    return copies


def early_kernel(weight, low, high, out, held, low_held, high_held, made, sem, write_sem):
    rows, columns = weight.shape
    part, tile = held.shape[0], min(columns, TILE)
    column = pl.multiple_of(lax.axis_index("fsdp") * rows, rows)

    @pl.when(first_chip())
    def _():
        size = part // 2 if part % 512 == 0 else part
        bands = [slice(start, start + size) for start in range(0, part, size)]
        smalls = [
            pltpu.make_async_copy(low, low_held, sem.at[0]),
            pltpu.make_async_copy(high, high_held, sem.at[1]),
        ]
        reads = [
            pltpu.make_async_copy(
                weight.at[pl.ds(band.start, size)], held.at[pl.ds(band.start, size)],
                sem.at[2 + k],
            )
            for k, band in enumerate(bands)
        ]
        for copy in smalls + reads:
            copy.start()
        for copy in smalls:
            copy.wait()
        writes = []
        for k, band in enumerate(bands):
            reads[k].wait()
            for j in range(columns // tile):
                piece = pl.ds(j * tile, tile)
                made[piece, band] = merge(held[band, piece], low_held[:, band], high_held[:, piece])
            writes.append(pltpu.make_async_copy(
                made.at[:, pl.ds(band.start, size)],
                out.at[:, pl.ds(column + band.start, size)], write_sem.at[k],
            ))
            writes[-1].start()
        for copy in writes:
            copy.wait()


def early_part(fsdp, weight, low, high):
    rows, columns = weight.shape
    rank, part = low.shape[0], early_rows(rows)
    dma = pltpu.SemaphoreType.DMA
    return pl.pallas_call(
        early_kernel,
        out_shape=jax.ShapeDtypeStruct((columns, rows * fsdp), jnp.bfloat16),
        in_specs=[HBM] * 3,
        out_specs=ANY,
        scratch_shapes=[
            pltpu.VMEM((part, columns), jnp.bfloat16),
            pltpu.VMEM((rank, rows), jnp.bfloat16),
            pltpu.VMEM((rank, columns), jnp.bfloat16),
            pltpu.VMEM((columns, part), jnp.bfloat16),
            dma((4,)), dma((2,)),
        ],
        compiler_params=pltpu.CompilerParams(vmem_limit_bytes=12 * MIB),
        cost_estimate=cost(rows * columns * rank, rows * columns),
    )(*[in_hbm(a) for a in (weight, low, high)])


def gate_kernel(fsdp, own_gate, own_up, high, *refs):
    theirs, (_, out_gate, out_up, made, own_sem, write_sem) = refs[:-6], refs[-6:]
    rows = own_gate.shape[1]
    part = early_rows(rows)
    mine = column_of(0, fsdp, rows)
    copies = [pltpu.make_async_copy(own_gate, out_gate.at[:, mine], own_sem.at[0])]
    if part < rows:
        second = pl.ds(pl.multiple_of(lax.axis_index("fsdp") * rows + part, part), rows - part)
        copies.append(pltpu.make_async_copy(
            own_up.at[:, pl.ds(part, rows - part)], out_up.at[:, second], own_sem.at[1]
        ))
    first = pl.ds(pl.multiple_of(lax.axis_index("fsdp") * rows, part), part)
    unwritten = pltpu.make_async_copy(
        own_up.at[:, pl.ds(0, part)], out_up.at[:, first], own_sem.at[2]
    )
    for copy in copies:
        copy.start()
    pl.when(jnp.logical_not(first_chip()))(unwritten.start)
    copies += merge_theirs(fsdp, theirs[::2], theirs[1::2], high, out_gate, made, write_sem)
    for copy in copies:
        copy.wait()
    pl.when(jnp.logical_not(first_chip()))(unwritten.wait)


def up_kernel(sizes, norm_all, high, *refs):
    fsdp, model = sizes
    theirs, (_, out, serve_norm, made, gain, held_norm, norm_sem, write_sem) = refs[:-8], refs[-8:]
    rank, size = high.shape[0], gain.shape[-1]
    row = lax.axis_index("fsdp")
    for k in range(model):
        gain[row * model + k] = norm_all[k, 0] + norm_all[k, 1]
    for step in range(1, fsdp):
        source = lax.rem(row + (fsdp - step), fsdp)
        pieces = theirs[2 * step - 1][rank:, :size].astype(jnp.float32)
        for k in range(model):
            gain[source * model + k] = pieces[k: k + 1]
    for k in range(fsdp * model):
        held_norm[pl.ds(k * size, size)] = gain[k, 0, :].astype(held_norm.dtype)
    copies = [pltpu.make_async_copy(held_norm, serve_norm, norm_sem)]
    copies[0].start()
    copies += merge_theirs(fsdp, theirs[::2], theirs[1::2], high, out, made, write_sem)
    for copy in copies:
        copy.wait()


def theirs_scratch(fsdp, columns, rows):
    return [
        pltpu.VMEM((fsdp - 1, columns, rows), jnp.bfloat16),
        pltpu.SemaphoreType.DMA((fsdp - 1, columns // min(columns, TILE))),
    ]


def gate_part(fsdp, own_gate, own_up, high, theirs, held):
    columns, rows = own_gate.shape
    full = jax.ShapeDtypeStruct((columns, rows * fsdp), jnp.bfloat16)
    operands = [own_gate, own_up, high, *theirs]
    made, sem = theirs_scratch(fsdp, columns, rows)
    return pl.pallas_call(
        functools.partial(gate_kernel, fsdp),
        out_shape=[full, full],
        in_specs=[VMEM] * len(operands) + [ANY],
        out_specs=[ANY, ANY],
        scratch_shapes=[made, pltpu.SemaphoreType.DMA((3,)), sem],
        input_output_aliases={len(operands): 1},
        compiler_params=pltpu.CompilerParams(vmem_limit_bytes=12 * MIB),
        cost_estimate=cost(2 * rows * columns * high.shape[0], 6 * rows * columns),
    )(*[in_vmem(a) for a in operands], held)


def up_part(sizes, norm_all, high, theirs, held):
    rows, columns = theirs[0].shape
    operands = [norm_all, high, *theirs]
    count = sizes[0] * sizes[1]
    norm = jax.ShapeDtypeStruct((count * norm_all.shape[-1],), jnp.bfloat16)
    made, sem = theirs_scratch(sizes[0], columns, rows)
    return pl.pallas_call(
        functools.partial(up_kernel, sizes),
        out_shape=[
            jax.ShapeDtypeStruct(held.shape, held.dtype),
            norm,
        ],
        in_specs=[VMEM] * len(operands) + [ANY],
        out_specs=[ANY, HBM],
        scratch_shapes=[
            made, pltpu.VMEM((count,) + norm_all.shape[2:], jnp.float32),
            pltpu.VMEM(norm.shape, norm.dtype), pltpu.SemaphoreType.DMA, sem,
        ],
        input_output_aliases={len(operands): 0},
        compiler_params=pltpu.CompilerParams(vmem_limit_bytes=12 * MIB),
        cost_estimate=cost(2 * rows * columns * high.shape[0], 2 * rows * columns),
    )(*[in_vmem(a) for a in operands], held)


def send(array, fsdp):
    return [
        lax.ppermute(array, "fsdp", [(i, (i + step) % fsdp) for i in range(fsdp)])
        for step in range(1, fsdp)
    ]


def paired(*lists):
    return [a for group in zip(*lists) for a in group]


def body(sizes, weight_gate, low_gate, high_gate, weight_up, low_up, high_up, norm_train, norm_step):
    fsdp, _ = sizes
    low_gate, low_up = low_gate.T, low_up.T
    its_gate = send(in_hbm(weight_gate), fsdp)
    its_low = send(in_hbm(low_gate), fsdp)
    its_up = send(in_hbm(weight_up), fsdp)
    groups = [(weight_gate, low_gate, high_gate), (weight_up, low_up, high_up)]
    up = early_part(fsdp, weight_up, low_up, high_up)
    norm_train, norm_step, up = lax.optimization_barrier((norm_train, norm_step, up))
    norms = [norm_train.reshape(1, -1), norm_step.reshape(1, -1)]
    norm_all, pack, own_gate, own_up = own_part(sizes, groups, norms)
    its_pack = send(pack, fsdp)
    gate, up = gate_part(fsdp, own_gate, own_up, high_gate, paired(its_gate, its_low), up)
    up, serve_norm = up_part(sizes, norm_all, high_up, paired(its_up, its_pack), up)
    return gate, up, serve_norm


def solution(mesh):
    whole = P(("ens", "fsdp", "model"))
    rows, thin, high = P(("ens", "fsdp"), "model"), P(("ens", "fsdp"), None), P("ens", "model")
    return jax.shard_map(
        functools.partial(body, (mesh.shape["fsdp"], mesh.shape["model"])),
        mesh=mesh,
        in_specs=(rows, thin, high, rows, thin, high, whole, whole),
        out_specs=(P(("ens", "model"), None), P(("ens", "model"), None), P("ens")),
        check_vma=False,
    )
```

```python
import functools

import jax
import jax.numpy as jnp
from jax import lax
from jax.experimental import pallas as pl
from jax.experimental.pallas import tpu as pltpu
from jax.sharding import PartitionSpec as P


mix_rate = 2.0
MIB = 2 ** 20
MESH = pl.DeviceIdType.MESH
VMEM, HBM = pl.BlockSpec(memory_space=pltpu.VMEM), pl.BlockSpec(memory_space=pltpu.HBM)
ANY = pl.BlockSpec(memory_space=pl.ANY)

TILE = 256
CUTS = ((2, 2), (1, 1, 2))
IN_FLIGHT = 3
EXTRA = 16


def in_vmem(array):
    return pltpu.with_memory_space_constraint(array, pltpu.VMEM)


def in_hbm(array):
    return pltpu.with_memory_space_constraint(array, pltpu.HBM)


def merge(weight, low, high):
    product = lax.dot_general(
        high, low * mix_rate, (((0,), (0,)), ((), ())), preferred_element_type=jnp.float32
    )
    return (weight.T.astype(jnp.float32) + product).astype(jnp.bfloat16)


def cost(flops, size):
    return pl.CostEstimate(flops=flops, bytes_accessed=size, transcendentals=0)


def first_chip():
    return lax.axis_index("ens") + lax.axis_index("model") == 0


def early_rows(rows):
    return rows // 2 if rows % 512 == 0 else rows


def blocks_of(rows):
    order = []
    for i in (1, 0):
        start = 0
        for cut in CUTS[i] if rows % 512 == 0 else (4,):
            order.append((i, start, rows * cut // 4))
            start += rows * cut // 4
    return order


def own_kernel(sizes, *refs):
    _, model = sizes
    ins, norms, (norm_all, pack, *outs) = refs[:6], refs[6:8], refs[8:12]
    held, low_held, high_held, read_sem, small_sem, keep_sem, send_sem, recv_sem = refs[12:]
    rows, columns = ins[0].shape
    column = lax.axis_index("model")
    barrier = pltpu.get_barrier_semaphore()

    def peer(shift):
        return {"model": lax.rem(column + shift, model)}

    peers = range(1, model)
    for shift in peers:
        pl.semaphore_signal(barrier, inc=1, device_id=peer(shift), device_id_type=MESH)

    keep = [
        pltpu.make_async_copy(norms[i], norm_all.at[column, i], keep_sem.at[i]) for i in range(2)
    ]
    smalls = [
        [
            pltpu.make_async_copy(ins[3 * i + 1], low_held.at[i], small_sem.at[i, 0]),
            pltpu.make_async_copy(ins[3 * i + 2], high_held.at[i], small_sem.at[i, 1]),
        ]
        for i in range(2)
    ]
    order = blocks_of(rows)
    reads = [
        pltpu.make_async_copy(
            ins[3 * i].at[pl.ds(start, size)], held.at[i, pl.ds(start, size)], read_sem.at[n]
        )
        for n, (i, start, size) in enumerate(order)
    ]
    for copy in smalls[1] + reads[:IN_FLIGHT] + keep + smalls[0]:
        copy.start()

    def pieces():
        return [
            pltpu.make_async_remote_copy(
                src_ref=norm_all.at[column], dst_ref=norm_all.at[column],
                send_sem=send_sem.at[shift], recv_sem=recv_sem.at[shift],
                device_id=peer(shift), device_id_type=MESH,
            )
            for shift in peers
        ]

    moment = jnp.minimum(jnp.maximum(3 - 6 * column // model, 0), len(order))

    def exchange(n):
        @pl.when(moment == n)
        def _():
            pl.semaphore_wait(barrier, len(peers))
            for copy in pieces():
                copy.start()

    for copy in keep:
        copy.wait()
    ahead = IN_FLIGHT
    ready = set()
    for n, (i, start, size) in enumerate(order):
        exchange(n)
        if i not in ready:
            for copy in smalls[i]:
                copy.wait()
            ready.add(i)
        reads[n].wait()
        if ahead < len(reads):
            reads[ahead].start()
            ahead += 1

        def merge_block(i=i, band=slice(start, start + size)):
            for first in range(0, columns, min(columns, TILE)):
                piece = slice(first, first + min(columns, TILE))
                outs[i][piece, band] = merge(
                    held[i, band, piece], low_held[i, :, band], high_held[i, :, piece]
                )

        if i == 1 and start + size <= early_rows(rows):
            pl.when(jnp.logical_not(first_chip()))(merge_block)
        else:
            merge_block()
    exchange(len(order))
    for copy in pieces():
        copy.wait()
    rank, size = low_held.shape[1], norm_all.shape[-1]
    pack[:rank] = low_held[1]
    rows_of = [norm_all[k, 0] + norm_all[k, 1] for k in range(model)]
    rows_of += [rows_of[-1]] * (pack.shape[0] - rank - model)
    pack[rank:, :size] = jnp.concatenate(rows_of, axis=0).astype(pack.dtype)


def own_part(sizes, groups, norms):
    _, model = sizes
    rows, columns = groups[0][0].shape
    rank = groups[0][1].shape[0]
    extra, dma = -(-model // EXTRA) * EXTRA, pltpu.SemaphoreType.DMA
    return pl.pallas_call(
        functools.partial(own_kernel, sizes),
        out_shape=[
            pltpu.VMEM((model, 2) + norms[0].shape, jnp.float32),
            pltpu.VMEM((rank + extra, rows), jnp.bfloat16),
            pltpu.VMEM((columns, rows), jnp.bfloat16),
            pltpu.VMEM((columns, rows), jnp.bfloat16),
        ],
        in_specs=[HBM] * 8,
        out_specs=[VMEM] * 4,
        scratch_shapes=[
            pltpu.VMEM((2, rows, columns), jnp.bfloat16),
            pltpu.VMEM((2, rank, rows), jnp.bfloat16),
            pltpu.VMEM((2, rank, columns), jnp.bfloat16),
            dma((len(blocks_of(rows)),)), dma((2, 2)), dma((2,)), dma((model,)), dma((model,)),
        ],
        compiler_params=pltpu.CompilerParams(
            collective_id=0, has_side_effects=True, vmem_limit_bytes=12 * MIB
        ),
        cost_estimate=cost(4 * rows * columns * rank, 4 * rows * columns),
    )(*[in_hbm(a) for group in groups for a in group], *[in_hbm(a) for a in norms])


def column_of(step, fsdp, rows):
    source = lax.rem(lax.axis_index("fsdp") + (fsdp - step), fsdp)
    return pl.ds(pl.multiple_of(source * rows, rows), rows)


def merge_theirs(fsdp, weights, lows, high, out, made, sem):
    copies = []
    rank = high.shape[0]
    for step, (weight, low) in enumerate(zip(weights, lows), 1):
        rows, columns = weight.shape
        tile = min(columns, TILE)
        for j in range(columns // tile):
            piece = pl.ds(j * tile, tile)
            made[step - 1, piece] = merge(weight[:, piece], low[:rank], high[:, piece])
            copies.append(pltpu.make_async_copy(
                made.at[step - 1, piece], out.at[piece, column_of(step, fsdp, rows)],
                sem.at[step - 1, j],
            ))
            copies[-1].start()
    return copies


def early_kernel(weight, low, high, out, held, low_held, high_held, made, sem, write_sem):
    rows, columns = weight.shape
    part, tile = held.shape[0], min(columns, TILE)
    column = pl.multiple_of(lax.axis_index("fsdp") * rows, rows)

    @pl.when(first_chip())
    def _():
        size = part // 2 if part % 256 == 0 else part
        bands = [slice(start, start + size) for start in range(0, part, size)]
        smalls = [
            pltpu.make_async_copy(low, low_held, sem.at[0]),
            pltpu.make_async_copy(high, high_held, sem.at[1]),
        ]
        reads = [
            pltpu.make_async_copy(
                weight.at[pl.ds(band.start, size)], held.at[pl.ds(band.start, size)],
                sem.at[2 + k],
            )
            for k, band in enumerate(bands)
        ]
        for copy in smalls + reads:
            copy.start()
        for copy in smalls:
            copy.wait()
        writes = []
        for k, band in enumerate(bands):
            reads[k].wait()
            for j in range(columns // tile):
                piece = pl.ds(j * tile, tile)
                made[piece, band] = merge(held[band, piece], low_held[:, band], high_held[:, piece])
            writes.append(pltpu.make_async_copy(
                made.at[:, pl.ds(band.start, size)],
                out.at[:, pl.ds(column + band.start, size)], write_sem.at[k],
            ))
            writes[-1].start()
        for copy in writes:
            copy.wait()


def early_part(fsdp, weight, low, high):
    rows, columns = weight.shape
    rank, part = low.shape[0], early_rows(rows)
    dma = pltpu.SemaphoreType.DMA
    return pl.pallas_call(
        early_kernel,
        out_shape=jax.ShapeDtypeStruct((columns, rows * fsdp), jnp.bfloat16),
        in_specs=[HBM] * 3,
        out_specs=ANY,
        scratch_shapes=[
            pltpu.VMEM((part, columns), jnp.bfloat16),
            pltpu.VMEM((rank, rows), jnp.bfloat16),
            pltpu.VMEM((rank, columns), jnp.bfloat16),
            pltpu.VMEM((columns, part), jnp.bfloat16),
            dma((4,)), dma((2,)),
        ],
        compiler_params=pltpu.CompilerParams(vmem_limit_bytes=12 * MIB),
        cost_estimate=cost(rows * columns * rank, rows * columns),
    )(*[in_hbm(a) for a in (weight, low, high)])


def gate_kernel(fsdp, own_gate, own_up, high, *refs):
    theirs, (_, out_gate, out_up, made, own_sem, write_sem) = refs[:-6], refs[-6:]
    rows = own_gate.shape[1]
    part = early_rows(rows)
    mine = column_of(0, fsdp, rows)
    copies = [pltpu.make_async_copy(own_gate, out_gate.at[:, mine], own_sem.at[0])]
    if part < rows:
        second = pl.ds(pl.multiple_of(lax.axis_index("fsdp") * rows + part, part), rows - part)
        copies.append(pltpu.make_async_copy(
            own_up.at[:, pl.ds(part, rows - part)], out_up.at[:, second], own_sem.at[1]
        ))
    first = pl.ds(pl.multiple_of(lax.axis_index("fsdp") * rows, part), part)
    unwritten = pltpu.make_async_copy(
        own_up.at[:, pl.ds(0, part)], out_up.at[:, first], own_sem.at[2]
    )
    for copy in copies:
        copy.start()
    pl.when(jnp.logical_not(first_chip()))(unwritten.start)
    copies += merge_theirs(fsdp, theirs[::2], theirs[1::2], high, out_gate, made, write_sem)
    for copy in copies:
        copy.wait()
    pl.when(jnp.logical_not(first_chip()))(unwritten.wait)


def up_kernel(sizes, norm_all, high, *refs):
    fsdp, model = sizes
    theirs, (_, out, serve_norm, made, gain, held_norm, norm_sem, write_sem) = refs[:-8], refs[-8:]
    rank, size = high.shape[0], gain.shape[-1]
    copies = merge_theirs(fsdp, theirs[::2], theirs[1::2], high, out, made, write_sem)
    row = lax.axis_index("fsdp")
    for k in range(model):
        gain[row * model + k] = norm_all[k, 0] + norm_all[k, 1]
    for step in range(1, fsdp):
        source = lax.rem(row + (fsdp - step), fsdp)
        pieces = theirs[2 * step - 1][rank:, :size].astype(jnp.float32)
        for k in range(model):
            gain[source * model + k] = pieces[k: k + 1]
    for k in range(fsdp * model):
        held_norm[pl.ds(k * size, size)] = gain[k, 0, :].astype(held_norm.dtype)
    copies.append(pltpu.make_async_copy(held_norm, serve_norm, norm_sem))
    copies[-1].start()
    for copy in copies:
        copy.wait()


def theirs_scratch(fsdp, columns, rows):
    return [
        pltpu.VMEM((fsdp - 1, columns, rows), jnp.bfloat16),
        pltpu.SemaphoreType.DMA((fsdp - 1, columns // min(columns, TILE))),
    ]


def gate_part(fsdp, own_gate, own_up, high, theirs, held):
    columns, rows = own_gate.shape
    full = jax.ShapeDtypeStruct((columns, rows * fsdp), jnp.bfloat16)
    operands = [own_gate, own_up, high, *theirs]
    made, sem = theirs_scratch(fsdp, columns, rows)
    return pl.pallas_call(
        functools.partial(gate_kernel, fsdp),
        out_shape=[full, full],
        in_specs=[VMEM] * len(operands) + [ANY],
        out_specs=[ANY, ANY],
        scratch_shapes=[made, pltpu.SemaphoreType.DMA((3,)), sem],
        input_output_aliases={len(operands): 1},
        compiler_params=pltpu.CompilerParams(vmem_limit_bytes=12 * MIB),
        cost_estimate=cost(2 * rows * columns * high.shape[0], 6 * rows * columns),
    )(*[in_vmem(a) for a in operands], held)


def up_part(sizes, norm_all, high, theirs, held):
    rows, columns = theirs[0].shape
    operands = [norm_all, high, *theirs]
    count = sizes[0] * sizes[1]
    norm = jax.ShapeDtypeStruct((count * norm_all.shape[-1],), jnp.bfloat16)
    made, sem = theirs_scratch(sizes[0], columns, rows)
    return pl.pallas_call(
        functools.partial(up_kernel, sizes),
        out_shape=[
            jax.ShapeDtypeStruct(held.shape, held.dtype),
            norm,
        ],
        in_specs=[VMEM] * len(operands) + [ANY],
        out_specs=[ANY, HBM],
        scratch_shapes=[
            made, pltpu.VMEM((count,) + norm_all.shape[2:], jnp.float32),
            pltpu.VMEM(norm.shape, norm.dtype), pltpu.SemaphoreType.DMA, sem,
        ],
        input_output_aliases={len(operands): 0},
        compiler_params=pltpu.CompilerParams(vmem_limit_bytes=12 * MIB),
        cost_estimate=cost(2 * rows * columns * high.shape[0], 2 * rows * columns),
    )(*[in_vmem(a) for a in operands], held)


def send(array, fsdp):
    return [
        lax.ppermute(array, "fsdp", [(i, (i + step) % fsdp) for i in range(fsdp)])
        for step in range(1, fsdp)
    ]


def paired(*lists):
    return [a for group in zip(*lists) for a in group]


def body(sizes, weight_gate, low_gate, high_gate, weight_up, low_up, high_up, norm_train, norm_step):
    fsdp, _ = sizes
    low_gate, low_up = low_gate.T, low_up.T
    its_gate = send(in_hbm(weight_gate), fsdp)
    its_low = send(in_hbm(low_gate), fsdp)
    its_up = send(in_hbm(weight_up), fsdp)
    groups = [(weight_gate, low_gate, high_gate), (weight_up, low_up, high_up)]
    up = early_part(fsdp, weight_up, low_up, high_up)
    norm_train, norm_step, up = lax.optimization_barrier((norm_train, norm_step, up))
    norms = [norm_train.reshape(1, -1), norm_step.reshape(1, -1)]
    norm_all, pack, own_gate, own_up = own_part(sizes, groups, norms)
    its_pack = send(pack, fsdp)
    gate, up = gate_part(fsdp, own_gate, own_up, high_gate, paired(its_gate, its_low), up)
    up, serve_norm = up_part(sizes, norm_all, high_up, paired(its_up, its_pack), up)
    return gate, up, serve_norm


def solution(mesh):
    whole = P(("ens", "fsdp", "model"))
    rows, thin, high = P(("ens", "fsdp"), "model"), P(("ens", "fsdp"), None), P("ens", "model")
    return jax.shard_map(
        functools.partial(body, (mesh.shape["fsdp"], mesh.shape["model"])),
        mesh=mesh,
        in_specs=(rows, thin, high, rows, thin, high, whole, whole),
        out_specs=(P(("ens", "model"), None), P(("ens", "model"), None), P("ens")),
        check_vma=False,
    )
```
